128 devices in a mesh: expert: 4 (over z), shard: 32 (over y, x, core).
Axes of the slice: x: 4, y: 4, z: 4, core: 2. Of those that a mesh axis runs over, the one named last changes fastest.
Arguments:
- master_gate: float32 [64, 2048, 1024], P('expert', 'shard'), may hold values from -0.25 to 0.25
- second_gate: float32 [64, 2048, 1024], P('expert', 'shard'), may hold values from -0.125 to 0.125
- master_up: float32 [64, 2048, 1024], P('expert', 'shard'), may hold values from -0.25 to 0.25
- second_up: float32 [64, 2048, 1024], P('expert', 'shard'), may hold values from -0.125 to 0.125
- mix_share: float32 [64], P('expert'), may hold values from 0.2 to 0.8
- router_weight: float32 [2048, 64], P('shard', 'expert'), may hold values from -0.125 to 0.125
- router_gain: float32 [2048], P('shard'), may hold values from 0.25 to 1.75
Outputs:
- final_gate: bfloat16 [64, 2048, 1024], P('expert', None, 'shard')
- final_up: bfloat16 [64, 2048, 1024], P('expert', None, 'shard')
- scale_gate: float32 [64, 1024], P('expert', 'shard')
- scale_up: float32 [64, 1024], P('expert', 'shard')
- serve_router: bfloat16 [2048, 64], replicated
The draws below stay inside these ranges and needn't reach their ends.
All inputs are finite; a program needn't handle non-finite values.
Results may differ from the reference program's by a relative error of at most 0.001.
Values may be sent and summed in bfloat16 or wider, within the bound.
No kernel may reach another device: no remote copies, remote signals or barrier semaphores. Data moves between devices by JAX's collectives and lax.ppermute only.
A program may use at most 128 MiB of HBM per device.

```python
import jax
import jax.numpy as jnp

EXPERTS = 64
D_MODEL = 2048
D_EXPERT = 1024


def with_spikes(values, own_key, source, target, blocks, factor):
    def block_of(position):
        return (jnp.arange(values.shape[position]) // (values.shape[position] // blocks)).reshape((-1,) + (1,) * (values.ndim - 1 - position))

    first = jax.random.permutation(own_key, blocks)[block_of(target)]
    other_side = (block_of(target) + blocks // 2) % blocks
    return jnp.where((block_of(source) == first) | (block_of(source) == other_side), factor * values, values)


def block_scale(key, dims, cuts, low, top_value):
    factor_of, own = 1.0, jax.random.fold_in(key, 6)
    for axis_at, shards_of in cuts:
        draws = jnp.exp(jax.random.uniform(jax.random.fold_in(own, axis_at), (shards_of,), jnp.float32, low / len(cuts), top_value / len(cuts)))
        factor_of = factor_of * jnp.repeat(draws, dims[axis_at] // shards_of).reshape([-1 if axis == axis_at else 1 for axis in range(len(dims))])
    return factor_of


def normal_values(rng, extent, deviation, bound, shards=(), dtype=jnp.bfloat16):
    factor_of = block_scale(rng, extent, shards, -0.22, 0.18) if shards else 1.0
    array = jax.random.normal(rng, extent, jnp.float32) * deviation * factor_of
    return jnp.minimum(jnp.maximum(array, -bound), bound).astype(dtype)


def heavy_noise(rng, extent, spread, reach, pieces, heavy, dtype=jnp.bfloat16):
    drawn = spread * jax.random.normal(rng, extent, jnp.float32)
    if pieces:
        drawn = drawn * block_scale(rng, extent, pieces, -0.22, 0.18)
    return jnp.clip(with_spikes(drawn, jax.random.fold_in(rng, 3), *heavy), -reach, reach).astype(dtype)


def setup_inputs(seed: int = 0) -> dict:
    streams_of = jax.random.split(jax.random.key(seed), 8)
    master_gate = heavy_noise(streams_of[0], (EXPERTS, D_MODEL, D_EXPERT), D_MODEL ** -0.5, 0.25, ((0, 4), (1, 32)), (1, 2, 32, 2.75), jnp.float32)
    second_gate = normal_values(streams_of[1], (EXPERTS, D_MODEL, D_EXPERT), D_MODEL ** -0.5, 0.125, ((0, 4), (1, 32)), jnp.float32)
    master_up = heavy_noise(streams_of[2], (EXPERTS, D_MODEL, D_EXPERT), D_MODEL ** -0.5, 0.25, ((0, 4), (1, 32)), (1, 2, 32, 2.75), jnp.float32)
    second_up = normal_values(streams_of[3], (EXPERTS, D_MODEL, D_EXPERT), D_MODEL ** -0.5, 0.125, ((0, 4), (1, 32)), jnp.float32)
    mix_share = jnp.clip(0.2 + 0.6 * jax.random.uniform(streams_of[4], (EXPERTS,), jnp.float32) ** block_scale(streams_of[4], (EXPERTS,), ((0, 4),), -0.2, 0.2), 0.2, 0.8)
    router_weight = normal_values(streams_of[5], (D_MODEL, EXPERTS), D_MODEL ** -0.5, 0.125, ((0, 32), (1, 4)), jnp.float32)
    router_gain = jnp.clip(1.0 + 0.15 * jax.random.normal(streams_of[6], (D_MODEL,), jnp.float32), 0.25, 1.75)
    return {"master_gate": master_gate, "second_gate": second_gate, "master_up": master_up, "second_up": second_up, "mix_share": mix_share, "router_weight": router_weight, "router_gain": router_gain}


def reference(master_gate, second_gate, master_up, second_up, mix_share, router_weight, router_gain):
    merged_gate = mix_share[:, None, None] * master_gate + (1.0 - mix_share[:, None, None]) * second_gate
    merged_up = mix_share[:, None, None] * master_up + (1.0 - mix_share[:, None, None]) * second_up
    scale_gate = jnp.sum(jnp.abs(merged_gate), axis=1) / D_MODEL
    final_gate = (merged_gate / jnp.expand_dims(scale_gate, 1)).astype(jnp.bfloat16)
    scale_up = jnp.sum(jnp.abs(merged_up), axis=1) / D_MODEL
    final_up = (merged_up / jnp.expand_dims(scale_up, 1)).astype(jnp.bfloat16)
    serve_router = (router_weight * router_gain[:, None]).astype(jnp.bfloat16)
    return final_gate, final_up, scale_gate, scale_up, serve_router
```

```python
import jax
import jax.numpy as jnp
from jax import lax
from jax.experimental import pallas as pl
from jax.experimental.pallas import tpu as pltpu
from jax.sharding import PartitionSpec as P

D_MODEL = 2048
E, R, C, S = 16, 64, 1024, 32
W = C // S
PAIRS = E // 2
TP = 2 * PAIRS
CORE = [[2 * i, 2 * i + 1] for i in range(S // 2)]
ALONG_X = [[y * 8 + x * 2 + c for x in range(4)] for y in range(4) for c in range(2)]
ALONG_Y = [[y * 8 + x * 2 + c for y in range(4)] for x in range(4) for c in range(2)]


def lanes(shape):
    return lax.broadcasted_iota(jnp.int32, shape, 1)


def merge_kernel(mix, a_gate, b_gate, a_up, b_up, turned, sums, row_sums):
    pair = pl.program_id(0)
    sublane = lax.broadcasted_iota(jnp.int32, (8, 128), 0)
    for t, (a, b) in enumerate(((a_gate, b_gate), (a_up, b_up))):
        for j in range(C // 128):
            cols = slice(j * 128, (j + 1) * 128)
            halves = []
            for par in range(2):
                share = mix[2 * pair + par]
                m = share * a[par, :, cols] + (1.0 - share) * b[par, :, cols]
                row_sums[t * 2 + pair // 4, :, cols] = jnp.where(
                    sublane == (2 * pair + par) % 8,
                    jnp.sum(jnp.abs(m), axis=0, keepdims=True),
                    row_sums[t * 2 + pair // 4, :, cols],
                )
                halves.append(m)
            flipped = jnp.concatenate(halves, axis=0).T
            for dd in range(128 // W):
                turned[j * (128 // W) + dd, t * PAIRS + pair] = flipped[dd * W : (dd + 1) * W]

    @pl.when(pair == PAIRS - 1)
    def _():
        group = lanes((8, 128)) // W
        for j in range(C // 128):
            v = [row_sums[g, :, j * 128 : (j + 1) * 128] for g in range(4)]
            for dd in range(4):
                out = jnp.zeros((8, 128), jnp.float32)
                for g in range(4):
                    shift = ((g - dd) * W) % 128
                    moved = pltpu.roll(v[g], shift, 1) if shift else v[g]
                    out = jnp.where(group == g, moved, out)
                sums[j * 4 + dd] = out


def scale_kernel(parts, spread, scale_gate, scale_up):
    scale = jnp.sum(parts[...], axis=0) / D_MODEL
    for s in range(S):
        spread[s] = scale
    for g in range(4):
        out = scale_gate if g < 2 else scale_up
        out[(g % 2) * 8 : (g % 2) * 8 + 8, :] = scale[:, g * W : (g + 1) * W]


def pack_kernel(turned, scales, packed, inverse):
    step = pl.program_id(0)
    per = packed.shape[0]

    @pl.when(step == 0)
    def _():
        for h in range(2):
            block = scales[h * 16 : (h + 1) * 16].reshape(128, 128)
            inverse[h] = (1.0 / block).T

    half = lanes((W, 128)) // 64
    for dl in range(per):
        d = step * per + dl
        column = (d % 16) * 8
        for tp in range(TP):
            rows = slice((tp // 4) * W, (tp // 4 + 1) * W)
            index = half + (column + 2 * (tp % 4))
            factor = jnp.take_along_axis(
                inverse[d // 16, rows, :], index, axis=1, mode="promise_in_bounds"
            )
            packed[dl, tp * W : (tp + 1) * W, :] = (turned[d, tp] * factor).astype(jnp.bfloat16)


def join(first, second):
    return (
        jnp.concatenate([first[:, :64], second[:, :64]], axis=1),
        jnp.concatenate([first[:, 64:], second[:, 64:]], axis=1),
    )


def unpack_kernel(gate, up, out_gate, out_up):
    for k in range(S // 2):
        cols = slice(k * 128, (k + 1) * 128)
        for block, out in ((gate, out_gate), (up, out_up)):
            even, odd = join(block[2 * k], block[2 * k + 1])
            out[0, :, cols] = even
            out[1, :, cols] = odd


def whole():
    return pl.BlockSpec(memory_space=pltpu.VMEM)


def exchange(x, axis):
    return lax.all_to_all(x, axis, split_axis=0, concat_axis=0, tiled=True)


MIB = 1024 * 1024


def body(master_gate, second_gate, master_up, second_up, mix_share, router_weight, router_gain):
    pair_block = pl.BlockSpec((2, R, C), lambda i: (i, 0, 0))
    turned, sums = pl.pallas_call(
        merge_kernel,
        grid=(PAIRS,),
        in_specs=[pl.BlockSpec(memory_space=pltpu.SMEM)] + [pair_block] * 4,
        out_specs=[whole(), whole()],
        out_shape=[
            pltpu.VMEM((S, TP, W, 128), jnp.float32),
            pltpu.VMEM((S, 8, 128), jnp.float32),
        ],
        scratch_shapes=[pltpu.VMEM((4, 8, C), jnp.float32)],
        compiler_params=pltpu.CompilerParams(vmem_limit_bytes=30 * MIB),
        name="merge",
    )(
        *(
            pltpu.with_memory_space_constraint(x, pltpu.HBM)
            for x in (mix_share, master_gate, second_gate, master_up, second_up)
        ),
    )

    parts = exchange(sums, "shard")

    spread, scale_gate, scale_up = pl.pallas_call(
        scale_kernel,
        in_specs=[whole()],
        out_specs=[whole()] * 3,
        out_shape=[
            jax.ShapeDtypeStruct((S, 8, 128), jnp.float32),
            jax.ShapeDtypeStruct((E, W), jnp.float32),
            jax.ShapeDtypeStruct((E, W), jnp.float32),
        ],
        compiler_params=pltpu.CompilerParams(vmem_limit_bytes=4 * MIB),
        name="scale",
    )(parts)
    scales = exchange(spread, "shard")

    per = 4
    rows = TP * W
    packed = pl.pallas_call(
        pack_kernel,
        grid=(S // per,),
        in_specs=[whole()] * 2,
        out_specs=pl.BlockSpec((per, rows, 128), lambda i: (i, 0, 0)),
        out_shape=pltpu.HBM((S, rows, 128), jnp.bfloat16),
        scratch_shapes=[pltpu.VMEM((2, 128, 128), jnp.float32)],
        compiler_params=pltpu.CompilerParams(vmem_limit_bytes=24 * MIB),
        name="pack",
    )(turned, scales)

    arrived = exchange(packed, "shard")
    _, router_weight, router_gain = lax.optimization_barrier((packed, router_weight, router_gain))
    router = (router_weight.T * router_gain[None, :]).astype(jnp.bfloat16)
    router = lax.all_gather(router, "expert", axis=0, tiled=True)
    router = lax.all_gather(router, "shard", axis=1, tiled=True, axis_index_groups=CORE)
    router = lax.all_gather(router, "shard", axis=0, axis_index_groups=ALONG_X)
    router = lax.all_gather(router, "shard", axis=0, axis_index_groups=ALONG_Y)
    serve_router = router.reshape(S // 2, 4 * E, 128).transpose(1, 0, 2).reshape(4 * E, S * R)

    final_gate, final_up = pl.pallas_call(
        unpack_kernel,
        grid=(PAIRS,),
        in_specs=[
            pl.BlockSpec((S, W, 128), lambda i: (0, i, 0)),
            pl.BlockSpec((S, W, 128), lambda i: (0, PAIRS + i, 0)),
        ],
        out_specs=[
            pl.BlockSpec((2, W, S * R), lambda i: (i, 0, 0)),
            pl.BlockSpec((2, W, S * R), lambda i: (i, 0, 0)),
        ],
        out_shape=[
            jax.ShapeDtypeStruct((E, W, S * R), jnp.bfloat16),
            jax.ShapeDtypeStruct((E, W, S * R), jnp.bfloat16),
        ],
        compiler_params=pltpu.CompilerParams(vmem_limit_bytes=24 * MIB),
        name="unpack",
    )(arrived, arrived)
    return (
        final_gate.transpose(0, 2, 1),
        final_up.transpose(0, 2, 1),
        scale_gate,
        scale_up,
        serve_router.T,
    )


def solution(mesh):
    in_specs = (
        P("expert", "shard", None),
        P("expert", "shard", None),
        P("expert", "shard", None),
        P("expert", "shard", None),
        P("expert"),
        P("shard", "expert"),
        P("shard"),
    )
    out_specs = (
        P("expert", None, "shard"),
        P("expert", None, "shard"),
        P("expert", "shard"),
        P("expert", "shard"),
        P(),
    )
    return jax.shard_map(body, mesh=mesh, in_specs=in_specs, out_specs=out_specs, check_vma=False)
```

```python
import jax
import jax.numpy as jnp
from jax import lax
from jax.experimental import pallas as pl
from jax.experimental.pallas import tpu as pltpu
from jax.sharding import PartitionSpec as P

D_MODEL = 2048
E, R, C, S = 16, 64, 1024, 32
W = C // S
PAIRS = E // 2
TP = 2 * PAIRS
MIB = 1024 * 1024


def lanes(shape):
    return lax.broadcasted_iota(jnp.int32, shape, 1)


def regroup(blocks):
    group = lanes((8, 128)) // W
    out = []
    for a in range(4):
        tile = blocks[0]
        for b in range(4):
            shift = ((b - a) * W) % 128
            moved = pltpu.roll(blocks[b], shift, 1) if shift else blocks[b]
            tile = moved if b == 0 else jnp.where(group == b, moved, tile)
        out.append(tile)
    return out


def join(first, second):
    return (
        jnp.concatenate([first[:, :64], second[:, :64]], axis=1),
        jnp.concatenate([first[:, 64:], second[:, 64:]], axis=1),
    )


def merge_kernel(
    mix, a_gate, b_gate, a_up, b_up, router, gain, merged, sums, inputs, row_sums, sems
):
    def copy(k, source, pair):
        return pltpu.make_async_copy(
            source.at[pl.ds(2 * pair, 2)], inputs.at[k, pl.ds(2 * pair, 2)], sems.at[k, pair]
        )

    sources = (a_gate, b_gate, a_up, b_up)
    for pair in range(PAIRS):
        for k, source in enumerate(sources):
            copy(k, source, pair).start()

    served = router[...] * gain[...]
    served = jnp.concatenate([served[:8], served[8:]], axis=1)
    for s in range(S):
        sums[s, 8:, :] = served
    sublane = lax.broadcasted_iota(jnp.int32, (8, 128), 0)

    def step(pair, carry):
        for t in range(2):
            for k in (2 * t, 2 * t + 1):
                copy(k, sources[k], pair).wait()
            for par in range(2):
                e = 2 * pair + par
                share = mix[e]
                other = 1.0 - share
                for j in range(C // 128):
                    cols = slice(j * 128, (j + 1) * 128)
                    m = share * inputs[2 * t, e, :, cols] + other * inputs[2 * t + 1, e, :, cols]
                    merged[t * E + e, :, cols] = m
                    row_sums[t * 2 + pair // 4, :, cols] = jnp.where(
                        sublane == e % 8,
                        jnp.sum(jnp.abs(m), axis=0, keepdims=True),
                        row_sums[t * 2 + pair // 4, :, cols],
                    )
        return carry

    lax.fori_loop(0, PAIRS, step, 0)
    for j in range(C // 128):
        tiles = regroup([row_sums[g, :, j * 128 : (j + 1) * 128] for g in range(4)])
        for dd in range(4):
            sums[j * 4 + dd, :8, :] = tiles[dd]


def scale_kernel(parts, spread, scale_gate, scale_up):
    scale = jnp.sum(parts[:, :8, :], axis=0) / D_MODEL
    for s in range(S):
        spread[s] = scale
    for g in range(4):
        out = scale_gate if g < 2 else scale_up
        out[(g % 2) * 8 : (g % 2) * 8 + 8, :] = scale[:, g * W : (g + 1) * W]


def router_kernel(parts, out):
    for k in range(S // 2):
        low, high = join(parts[2 * k, 8:, :], parts[2 * k + 1, 8:, :])
        out[:, k * 128 : (k + 1) * 128] = jnp.concatenate([low, high], axis=0).astype(jnp.bfloat16)


def pack_kernel(merged, scales, packed, inverse, blocks, sems):
    for j in range(C // 128):
        tiles = regroup([scales[4 * j + dd] for dd in range(4)])
        for g in range(4):
            inverse[g, :, j * 128 : (j + 1) * 128] = 1.0 / tiles[g]

    def copy(j):
        rows = pl.ds(4 * j, 4)
        return pltpu.make_async_copy(blocks.at[rows], packed.at[rows], sems.at[j])

    def step(j, carry):
        cols = pl.ds(pl.multiple_of(j * 128, 128), 128)
        for tp in range(TP):
            halves = []
            for par in range(2):
                te = 2 * tp + par
                factor = inverse[te // 8, te % 8 : te % 8 + 1, cols]
                halves.append((merged[te, :, cols] * factor).astype(jnp.bfloat16))
            turned = jnp.concatenate(halves, axis=0).T
            for dd in range(4):
                blocks[4 * j + dd, tp * W : (tp + 1) * W, :] = turned[dd * W : (dd + 1) * W]
        copy(j).start()
        return carry

    lax.fori_loop(0, C // 128, step, 0)
    for j in range(C // 128):
        copy(j).wait()


def unpack_kernel(arrived, out_gate, out_up, blocks, joined, in_sems, out_sems):
    def fetch(tp):
        rows = pl.ds(pl.multiple_of(tp * W, W), W)
        return pltpu.make_async_copy(arrived.at[:, rows], blocks.at[tp], in_sems.at[tp])

    def give(t, p):
        out = (out_gate, out_up)[t]
        return pltpu.make_async_copy(
            joined.at[t, pl.ds(2 * p, 2)], out.at[pl.ds(2 * p, 2)], out_sems.at[t, p]
        )

    for p in range(PAIRS):
        for t in range(2):
            fetch(t * PAIRS + p).start()

    def step(p, carry):
        for t in range(2):
            tp = t * PAIRS + p
            fetch(tp).wait()
            for k in range(S // 2):
                cols = slice(k * 128, (k + 1) * 128)
                even, odd = join(blocks[tp, 2 * k], blocks[tp, 2 * k + 1])
                joined[t, 2 * p, :, cols] = even
                joined[t, 2 * p + 1, :, cols] = odd
            give(t, p).start()
        return carry

    lax.fori_loop(0, PAIRS, step, 0)
    for p in range(PAIRS):
        for t in range(2):
            give(t, p).wait()


def whole():
    return pl.BlockSpec(memory_space=pltpu.VMEM)


def remote():
    return pl.BlockSpec(memory_space=pltpu.HBM)


def params(mib):
    return pltpu.CompilerParams(vmem_limit_bytes=mib * MIB)


def exchange(x):
    return lax.all_to_all(x, "shard", split_axis=0, concat_axis=0, tiled=True)


def body(master_gate, second_gate, master_up, second_up, mix_share, router_weight, router_gain):
    merged, sums = pl.pallas_call(
        merge_kernel,
        in_specs=[pl.BlockSpec(memory_space=pltpu.SMEM)] + [remote()] * 4 + [whole()] * 2,
        out_specs=[whole(), whole()],
        out_shape=[
            pltpu.VMEM((2 * E, R, C), jnp.float32),
            pltpu.VMEM((S, 16, 128), jnp.float32),
        ],
        scratch_shapes=[
            pltpu.VMEM((4, E, R, C), jnp.float32),
            pltpu.VMEM((4, 8, C), jnp.float32),
            pltpu.SemaphoreType.DMA((4, PAIRS)),
        ],
        compiler_params=params(20),
        name="merge",
    )(
        *(
            pltpu.with_memory_space_constraint(x, pltpu.HBM)
            for x in (mix_share, master_gate, second_gate, master_up, second_up)
        ),
        pltpu.with_memory_space_constraint(router_weight.T, pltpu.HBM),
        pltpu.with_memory_space_constraint(router_gain[None, :], pltpu.HBM),
    )

    parts = exchange(sums)

    spread, scale_gate, scale_up = pl.pallas_call(
        scale_kernel,
        in_specs=[whole()],
        out_specs=[whole()] * 3,
        out_shape=[
            jax.ShapeDtypeStruct((S, 8, 128), jnp.float32),
            jax.ShapeDtypeStruct((E, W), jnp.float32),
            jax.ShapeDtypeStruct((E, W), jnp.float32),
        ],
        compiler_params=params(4),
        name="scale",
    )(parts)
    scales = exchange(spread)

    packed = pl.pallas_call(
        pack_kernel,
        in_specs=[whole(), whole()],
        out_specs=remote(),
        out_shape=pltpu.HBM((S, TP * W, 128), jnp.bfloat16),
        scratch_shapes=[
            pltpu.VMEM((4, 8, C), jnp.float32),
            pltpu.VMEM((S, TP * W, 128), jnp.bfloat16),
            pltpu.SemaphoreType.DMA((C // 128,)),
        ],
        compiler_params=params(8),
        name="pack",
    )(merged, scales)

    arrived = exchange(packed)

    _, parts = lax.optimization_barrier((packed, parts))
    router = pl.pallas_call(
        router_kernel,
        in_specs=[whole()],
        out_specs=whole(),
        out_shape=jax.ShapeDtypeStruct((E, S * R), jnp.bfloat16),
        compiler_params=params(2),
        name="router",
    )(parts)
    serve_router = lax.all_gather(router, "expert", axis=0, tiled=True)

    final_gate, final_up = pl.pallas_call(
        unpack_kernel,
        in_specs=[remote()],
        out_specs=[remote(), remote()],
        out_shape=[jax.ShapeDtypeStruct((E, W, S * R), jnp.bfloat16)] * 2,
        scratch_shapes=[
            pltpu.VMEM((TP, S, W, 128), jnp.bfloat16),
            pltpu.VMEM((2, E, W, S * R), jnp.bfloat16),
            pltpu.SemaphoreType.DMA((TP,)),
            pltpu.SemaphoreType.DMA((2, PAIRS)),
        ],
        compiler_params=params(12),
        name="unpack",
    )(arrived)
    return (
        final_gate.transpose(0, 2, 1),
        final_up.transpose(0, 2, 1),
        scale_gate,
        scale_up,
        serve_router.T,
    )


def solution(mesh):
    in_specs = (
        P("expert", "shard", None),
        P("expert", "shard", None),
        P("expert", "shard", None),
        P("expert", "shard", None),
        P("expert"),
        P("shard", "expert"),
        P("shard"),
    )
    out_specs = (
        P("expert", None, "shard"),
        P("expert", None, "shard"),
        P("expert", "shard"),
        P("expert", "shard"),
        P(),
    )
    return jax.shard_map(body, mesh=mesh, in_specs=in_specs, out_specs=out_specs, check_vma=False)
```

```python
import jax
import jax.numpy as jnp
from jax import lax
from jax.experimental import pallas as pl
from jax.experimental.pallas import tpu as pltpu
from jax.sharding import PartitionSpec as P

D_MODEL = 2048
E, R, C, S = 16, 64, 1024, 32
W = C // S
PAIRS = E // 2
TP = 2 * PAIRS
MIB = 1024 * 1024
ORDER = [13, 3, 31, 6, 26, 27, 11, 25, 4, 18, 9, 17, 30, 0, 16, 15, 7, 12, 24, 1, 5, 23, 22, 28, 10, 20, 19, 8, 2, 21, 14, 29]
PLACE = [ORDER.index(s) for s in range(S)]


def lanes(shape):
    return lax.broadcasted_iota(jnp.int32, shape, 1)


def regroup(blocks):
    group = lanes((8, 128)) // W
    out = []
    for a in range(4):
        tile = blocks[0]
        for b in range(4):
            shift = ((b - a) * W) % 128
            moved = pltpu.roll(blocks[b], shift, 1) if shift else blocks[b]
            tile = moved if b == 0 else jnp.where(group == b, moved, tile)
        out.append(tile)
    return out


def join(first, second):
    return (
        jnp.concatenate([first[:, :64], second[:, :64]], axis=1),
        jnp.concatenate([first[:, 64:], second[:, 64:]], axis=1),
    )


def merge_kernel(
    mix, a_gate, b_gate, a_up, b_up, router, gain, merged, sums, inputs, row_sums, sems
):
    def copy(k, source, pair):
        return pltpu.make_async_copy(
            source.at[pl.ds(2 * pair, 2)], inputs.at[k, pl.ds(2 * pair, 2)], sems.at[k, pair]
        )

    sources = (a_gate, b_gate, a_up, b_up)
    for pair in range(PAIRS):
        for k, source in enumerate(sources):
            copy(k, source, pair).start()

    served = router[...] * gain[...]
    served = jnp.concatenate([served[:8], served[8:]], axis=1)
    for s in range(S):
        sums[s, 8:, :] = served
    sublane = lax.broadcasted_iota(jnp.int32, (8, 128), 0)

    def step(pair, carry):
        for t in range(2):
            for k in (2 * t, 2 * t + 1):
                copy(k, sources[k], pair).wait()
            for par in range(2):
                e = 2 * pair + par
                share = mix[e]
                other = 1.0 - share
                for j in range(C // 128):
                    cols = slice(j * 128, (j + 1) * 128)
                    m = share * inputs[2 * t, e, :, cols] + other * inputs[2 * t + 1, e, :, cols]
                    merged[t * E + e, :, cols] = m
                    row_sums[t * 2 + pair // 4, :, cols] = jnp.where(
                        sublane == e % 8,
                        jnp.sum(jnp.abs(m), axis=0, keepdims=True),
                        row_sums[t * 2 + pair // 4, :, cols],
                    )
        return carry

    lax.fori_loop(0, PAIRS, step, 0)
    for j in range(C // 128):
        tiles = regroup([row_sums[g, :, j * 128 : (j + 1) * 128] for g in range(4)])
        for dd in range(4):
            sums[PLACE[j * 4 + dd], :8, :] = tiles[dd]


def scale_kernel(parts, spread, scale_gate, scale_up):
    scale = jnp.sum(parts[:, :8, :], axis=0) / D_MODEL
    for s in range(S):
        spread[s] = scale
    for g in range(4):
        out = scale_gate if g < 2 else scale_up
        out[(g % 2) * 8 : (g % 2) * 8 + 8, :] = scale[:, g * W : (g + 1) * W]


def router_kernel(parts, out):
    for k in range(S // 2):
        low, high = join(parts[PLACE[2 * k], 8:, :], parts[PLACE[2 * k + 1], 8:, :])
        out[:, k * 128 : (k + 1) * 128] = jnp.concatenate([low, high], axis=0).astype(jnp.bfloat16)


def pack_kernel(merged, scales, packed, inverse, blocks, sems):
    for j in range(C // 128):
        tiles = regroup([scales[PLACE[4 * j + dd]] for dd in range(4)])
        for g in range(4):
            inverse[g, :, j * 128 : (j + 1) * 128] = 1.0 / tiles[g]

    def copy(d):
        return pltpu.make_async_copy(blocks.at[PLACE[d]], packed.at[PLACE[d]], sems.at[d])

    for j in range(C // 128):
        cols = slice(j * 128, (j + 1) * 128)
        for tp in range(TP):
            halves = []
            for par in range(2):
                te = 2 * tp + par
                factor = inverse[te // 8, te % 8 : te % 8 + 1, cols]
                halves.append((merged[te, :, cols] * factor).astype(jnp.bfloat16))
            turned = jnp.concatenate(halves, axis=0).T
            for dd in range(4):
                rows = slice(tp * W, (tp + 1) * W)
                blocks[PLACE[4 * j + dd], rows, :] = turned[dd * W : (dd + 1) * W]
        for dd in range(4):
            copy(4 * j + dd).start()
    for d in range(S):
        copy(d).wait()


def unpack_kernel(
    arrived, router, out_gate, out_up, out_router, blocks, joined, in_sems, out_sems, router_sem
):
    def fetch(tp):
        rows = pl.ds(pl.multiple_of(tp * W, W), W)
        return pltpu.make_async_copy(arrived.at[:, rows], blocks.at[tp], in_sems.at[tp])

    def give(t, p):
        out = (out_gate, out_up)[t]
        return pltpu.make_async_copy(
            joined.at[t, pl.ds(2 * p, 2)], out.at[pl.ds(2 * p, 2)], out_sems.at[t, p]
        )

    for p in range(PAIRS):
        for t in range(2):
            fetch(t * PAIRS + p).start()
    served = pltpu.make_async_copy(router, out_router, router_sem)
    served.start()

    def step(p, carry):
        for t in range(2):
            tp = t * PAIRS + p
            fetch(tp).wait()
            for k in range(S // 2):
                cols = slice(k * 128, (k + 1) * 128)
                even, odd = join(blocks[tp, PLACE[2 * k]], blocks[tp, PLACE[2 * k + 1]])
                joined[t, 2 * p, :, cols] = even
                joined[t, 2 * p + 1, :, cols] = odd
            give(t, p).start()
        return carry

    lax.fori_loop(0, PAIRS, step, 0)
    for p in range(PAIRS):
        for t in range(2):
            give(t, p).wait()
    served.wait()


def whole():
    return pl.BlockSpec(memory_space=pltpu.VMEM)


def remote():
    return pl.BlockSpec(memory_space=pltpu.HBM)


def params(mib):
    return pltpu.CompilerParams(vmem_limit_bytes=mib * MIB)


def exchange(x):
    return lax.all_to_all(
        x, "shard", split_axis=0, concat_axis=0, tiled=True, axis_index_groups=[ORDER]
    )


def body(master_gate, second_gate, master_up, second_up, mix_share, router_weight, router_gain):
    merged, sums = pl.pallas_call(
        merge_kernel,
        in_specs=[pl.BlockSpec(memory_space=pltpu.SMEM)] + [remote()] * 4 + [whole()] * 2,
        out_specs=[whole(), whole()],
        out_shape=[
            pltpu.VMEM((2 * E, R, C), jnp.float32),
            pltpu.VMEM((S, 16, 128), jnp.float32),
        ],
        scratch_shapes=[
            pltpu.VMEM((4, E, R, C), jnp.float32),
            pltpu.VMEM((4, 8, C), jnp.float32),
            pltpu.SemaphoreType.DMA((4, PAIRS)),
        ],
        compiler_params=params(20),
        name="merge",
    )(
        *(
            pltpu.with_memory_space_constraint(x, pltpu.HBM)
            for x in (mix_share, master_gate, second_gate, master_up, second_up)
        ),
        pltpu.with_memory_space_constraint(router_weight.T, pltpu.HBM),
        pltpu.with_memory_space_constraint(router_gain[None, :], pltpu.HBM),
    )

    parts = exchange(sums)

    spread, scale_gate, scale_up = pl.pallas_call(
        scale_kernel,
        in_specs=[whole()],
        out_specs=[whole()] * 3,
        out_shape=[
            jax.ShapeDtypeStruct((S, 8, 128), jnp.float32),
            jax.ShapeDtypeStruct((E, W), jnp.float32),
            jax.ShapeDtypeStruct((E, W), jnp.float32),
        ],
        compiler_params=params(4),
        name="scale",
    )(parts)
    scales = exchange(spread)

    packed = pl.pallas_call(
        pack_kernel,
        in_specs=[whole(), whole()],
        out_specs=remote(),
        out_shape=pltpu.HBM((S, TP * W, 128), jnp.bfloat16),
        scratch_shapes=[
            pltpu.VMEM((4, 8, C), jnp.float32),
            pltpu.VMEM((S, TP * W, 128), jnp.bfloat16),
            pltpu.SemaphoreType.DMA((S,)),
        ],
        compiler_params=params(8),
        name="pack",
    )(merged, scales)

    arrived = exchange(packed)

    _, parts = lax.optimization_barrier((packed, parts))
    router = pl.pallas_call(
        router_kernel,
        in_specs=[whole()],
        out_specs=whole(),
        out_shape=jax.ShapeDtypeStruct((E, S * R), jnp.bfloat16),
        compiler_params=params(2),
        name="router",
    )(parts)
    router = lax.all_gather(router, "expert", axis=0, tiled=True)

    final_gate, final_up, serve_router = pl.pallas_call(
        unpack_kernel,
        in_specs=[remote(), whole()],
        out_specs=[remote()] * 3,
        out_shape=[jax.ShapeDtypeStruct((E, W, S * R), jnp.bfloat16)] * 2
        + [jax.ShapeDtypeStruct((4 * E, S * R), jnp.bfloat16)],
        scratch_shapes=[
            pltpu.VMEM((TP, S, W, 128), jnp.bfloat16),
            pltpu.VMEM((2, E, W, S * R), jnp.bfloat16),
            pltpu.SemaphoreType.DMA((TP,)),
            pltpu.SemaphoreType.DMA((2, PAIRS)),
            pltpu.SemaphoreType.DMA,
        ],
        compiler_params=params(12),
        name="unpack",
    )(arrived, router)
    return (
        final_gate.transpose(0, 2, 1),
        final_up.transpose(0, 2, 1),
        scale_gate,
        scale_up,
        serve_router.T,
    )


def solution(mesh):
    in_specs = (
        P("expert", "shard", None),
        P("expert", "shard", None),
        P("expert", "shard", None),
        P("expert", "shard", None),
        P("expert"),
        P("shard", "expert"),
        P("shard"),
    )
    out_specs = (
        P("expert", None, "shard"),
        P("expert", None, "shard"),
        P("expert", "shard"),
        P("expert", "shard"),
        P(),
    )
    return jax.shard_map(body, mesh=mesh, in_specs=in_specs, out_specs=out_specs, check_vma=False)
```

```python
import jax
import jax.numpy as jnp
from jax import lax
from jax.experimental import pallas as pl
from jax.experimental.pallas import tpu as pltpu
from jax.sharding import PartitionSpec as P


D_MODEL = 2048
E, R, C, S = 16, 64, 1024, 32
W = C // S
PAIRS = E // 2
TP = 2 * PAIRS
MIB = 1024 * 1024
ORDER = [13, 3, 31, 6, 26, 27, 11, 25, 4, 18, 9, 17, 30, 0, 16, 15, 7, 12, 24, 1, 5, 23, 22, 28, 10, 20, 19, 8, 2, 21, 14, 29]
PLACE = [ORDER.index(s) for s in range(S)]


def lanes(shape):
    return lax.broadcasted_iota(jnp.int32, shape, 1)


def regroup(blocks):
    group = lanes((8, 128)) // W
    out = []
    for a in range(4):
        tile = blocks[0]
        for b in range(4):
            shift = ((b - a) * W) % 128
            moved = pltpu.roll(blocks[b], shift, 1) if shift else blocks[b]
            tile = moved if b == 0 else jnp.where(group == b, moved, tile)
        out.append(tile)
    return out


def join(first, second):
    return (
        jnp.concatenate([first[:, :64], second[:, :64]], axis=1),
        jnp.concatenate([first[:, 64:], second[:, 64:]], axis=1),
    )


def merge_kernel(mix, a_gate, b_gate, a_up, b_up, merged, sums, inputs, row_sums, sems):
    def copy(k, source, pair):
        return pltpu.make_async_copy(
            source.at[pl.ds(2 * pair, 2)], inputs.at[k, pl.ds(2 * pair, 2)], sems.at[k, pair]
        )

    sources = (a_gate, b_gate, a_up, b_up)
    for pair in range(PAIRS):
        for k, source in enumerate(sources):
            copy(k, source, pair).start()

    sublane = lax.broadcasted_iota(jnp.int32, (8, 128), 0)

    def step(pair, carry):
        for t in range(2):
            for k in (2 * t, 2 * t + 1):
                copy(k, sources[k], pair).wait()
            for par in range(2):
                e = 2 * pair + par
                share = mix[e]
                other = 1.0 - share
                for j in range(C // 128):
                    cols = slice(j * 128, (j + 1) * 128)
                    m = share * inputs[2 * t, e, :, cols] + other * inputs[2 * t + 1, e, :, cols]
                    merged[t * E + e, :, cols] = m
                    row_sums[t * 2 + pair // 4, :, cols] = jnp.where(
                        sublane == e % 8,
                        jnp.sum(jnp.abs(m), axis=0, keepdims=True),
                        row_sums[t * 2 + pair // 4, :, cols],
                    )
        return carry

    lax.fori_loop(0, PAIRS, step, 0)
    for j in range(C // 128):
        tiles = regroup([row_sums[g, :, j * 128 : (j + 1) * 128] for g in range(4)])
        for dd in range(4):
            sums[PLACE[j * 4 + dd]] = tiles[dd]


def scale_kernel(parts, spread, scale_gate, scale_up):
    scale = jnp.sum(parts[...], axis=0) / D_MODEL
    for s in range(S):
        spread[s] = scale
    for g in range(4):
        out = scale_gate if g < 2 else scale_up
        out[(g % 2) * 8 : (g % 2) * 8 + 8, :] = scale[:, g * W : (g + 1) * W]


def pack_kernel(merged, scales, gain, r0, r1, r2, r3, packed, inverse):
    for k, weight in enumerate((r0, r1, r2, r3)):
        served = weight[...] * gain[...]
        served = jnp.concatenate([served[:8], served[8:]], axis=1).astype(jnp.bfloat16)
        for d in range(S):
            packed[d, TP * W + 8 * k : TP * W + 8 * k + 8, :] = served
    for j in range(C // 128):
        tiles = regroup([scales[PLACE[4 * j + dd]] for dd in range(4)])
        for g in range(4):
            inverse[g, :, j * 128 : (j + 1) * 128] = 1.0 / tiles[g]

    for j in range(C // 128):
        cols = slice(j * 128, (j + 1) * 128)
        for tp in range(TP):
            halves = []
            for par in range(2):
                te = 2 * tp + par
                factor = inverse[te // 8, te % 8 : te % 8 + 1, cols]
                halves.append((merged[te, :, cols] * factor).astype(jnp.bfloat16))
            turned = jnp.concatenate(halves, axis=0).T
            for dd in range(4):
                rows = slice(tp * W, (tp + 1) * W)
                packed[PLACE[4 * j + dd], rows, :] = turned[dd * W : (dd + 1) * W]


def unpack_kernel(
    arrived, out_gate, out_up, out_router, joined, router, out_sems, router_sems
):
    me = lax.axis_index("expert")

    def serve(k):
        rows = pl.ds(pl.multiple_of(lax.rem(me + 4 - k, 4) * E, E), E)
        return pltpu.make_async_copy(router.at[k], out_router.at[rows], router_sems.at[k])

    def give(t, p):
        out = (out_gate, out_up)[t]
        return pltpu.make_async_copy(
            joined.at[t, pl.ds(2 * p, 2)], out.at[pl.ds(2 * p, 2)], out_sems.at[t, p]
        )

    def step(p, carry):
        for t in range(2):
            rows = pl.ds(pl.multiple_of((t * PAIRS + p) * W, W), W)
            for k in range(S // 2):
                cols = slice(k * 128, (k + 1) * 128)
                even, odd = join(arrived[PLACE[2 * k], rows], arrived[PLACE[2 * k + 1], rows])
                joined[t, 2 * p, :, cols] = even
                joined[t, 2 * p + 1, :, cols] = odd
            give(t, p).start()
        return carry

    lax.fori_loop(0, PAIRS, step, 0)
    for k in range(4):
        rows = slice(TP * W + 8 * k, TP * W + 8 * k + 8)
        for c in range(S // 2):
            low, high = join(arrived[PLACE[2 * c], rows], arrived[PLACE[2 * c + 1], rows])
            router[k, :8, c * 128 : (c + 1) * 128] = low
            router[k, 8:, c * 128 : (c + 1) * 128] = high
        serve(k).start()
    for p in range(PAIRS):
        for t in range(2):
            give(t, p).wait()
    for k in range(4):
        serve(k).wait()


def whole():
    return pl.BlockSpec(memory_space=pltpu.VMEM)


def remote():
    return pl.BlockSpec(memory_space=pltpu.HBM)


def params(mib):
    return pltpu.CompilerParams(vmem_limit_bytes=mib * MIB)


def exchange(x):
    return lax.all_to_all(
        x, "shard", split_axis=0, concat_axis=0, tiled=True, axis_index_groups=[ORDER]
    )


def serve_step(master_gate, second_gate, master_up, second_up, mix_share, router_weight, router_gain):
    weight = router_weight.T
    hops = [
        lax.ppermute(weight, "expert", [(z, (z + k) % 4) for z in range(4)])
        for k in range(1, 4)
    ]

    merged, sums = pl.pallas_call(
        merge_kernel,
        in_specs=[pl.BlockSpec(memory_space=pltpu.SMEM)] + [remote()] * 4,
        out_specs=[whole(), whole()],
        out_shape=[
            pltpu.VMEM((2 * E, R, C), jnp.float32),
            pltpu.VMEM((S, 8, 128), jnp.float32),
        ],
        scratch_shapes=[
            pltpu.VMEM((4, E, R, C), jnp.float32),
            pltpu.VMEM((4, 8, C), jnp.float32),
            pltpu.SemaphoreType.DMA((4, PAIRS)),
        ],
        compiler_params=params(20),
        name="merge",
    )(
        *(
            pltpu.with_memory_space_constraint(x, pltpu.HBM)
            for x in (mix_share, master_gate, second_gate, master_up, second_up)
        ),
    )

    parts = exchange(sums)

    spread, scale_gate, scale_up = pl.pallas_call(
        scale_kernel,
        in_specs=[whole()],
        out_specs=[whole()] * 3,
        out_shape=[
            jax.ShapeDtypeStruct((S, 8, 128), jnp.float32),
            jax.ShapeDtypeStruct((E, W), jnp.float32),
            jax.ShapeDtypeStruct((E, W), jnp.float32),
        ],
        compiler_params=params(4),
        name="scale",
    )(parts)
    scales = exchange(spread)

    rows = TP * W + 4 * E // 2
    packed = pl.pallas_call(
        pack_kernel,
        in_specs=[whole()] * 7,
        out_specs=whole(),
        out_shape=pltpu.VMEM((S, rows, 128), jnp.bfloat16),
        scratch_shapes=[pltpu.VMEM((4, 8, C), jnp.float32)],
        compiler_params=params(4),
        name="pack",
    )(merged, scales, router_gain[None, :], weight, *hops)
    arrived = pltpu.with_memory_space_constraint(exchange(packed), pltpu.VMEM)

    final_gate, final_up, serve_router = pl.pallas_call(
        unpack_kernel,
        in_specs=[whole()],
        out_specs=[remote()] * 3,
        out_shape=[jax.ShapeDtypeStruct((E, W, S * R), jnp.bfloat16)] * 2
        + [jax.ShapeDtypeStruct((4 * E, S * R), jnp.bfloat16)],
        scratch_shapes=[
            pltpu.VMEM((2, E, W, S * R), jnp.bfloat16),
            pltpu.VMEM((4, E, S * R), jnp.bfloat16),
            pltpu.SemaphoreType.DMA((2, PAIRS)),
            pltpu.SemaphoreType.DMA((4,)),
        ],
        compiler_params=params(10),
        name="unpack",
    )(arrived)
    return (
        final_gate.transpose(0, 2, 1),
        final_up.transpose(0, 2, 1),
        scale_gate,
        scale_up,
        serve_router.T,
    )


def solution(mesh):
    in_specs = (
        P("expert", "shard", None),
        P("expert", "shard", None),
        P("expert", "shard", None),
        P("expert", "shard", None),
        P("expert"),
        P("shard", "expert"),
        P("shard"),
    )
    out_specs = (
        P("expert", None, "shard"),
        P("expert", None, "shard"),
        P("expert", "shard"),
        P("expert", "shard"),
        P(),
    )
    return jax.shard_map(serve_step, mesh=mesh, in_specs=in_specs, out_specs=out_specs, check_vma=False)
```

```python
import jax
import jax.numpy as jnp
from jax import lax
from jax.experimental import pallas as pl
from jax.experimental.pallas import tpu as pltpu
from jax.sharding import PartitionSpec as P


D_MODEL = 2048
E, R, C, S = 16, 64, 1024, 32
W = C // S
PAIRS = E // 2
TP = 2 * PAIRS
MIB = 1024 * 1024
ORDER = [13, 3, 31, 6, 26, 27, 11, 25, 4, 18, 9, 17, 30, 0, 16, 15, 7, 12, 24, 1, 5, 23, 22, 28, 10, 20, 19, 8, 2, 21, 14, 29]
PLACE = [ORDER.index(s) for s in range(S)]


def lanes(shape):
    return lax.broadcasted_iota(jnp.int32, shape, 1)


def regroup(blocks):
    group = lanes((8, 128)) // W
    out = []
    for a in range(4):
        tile = blocks[0]
        for b in range(4):
            shift = ((b - a) * W) % 128
            moved = pltpu.roll(blocks[b], shift, 1) if shift else blocks[b]
            tile = moved if b == 0 else jnp.where(group == b, moved, tile)
        out.append(tile)
    return out


def join(first, second):
    return (
        jnp.concatenate([first[:, :64], second[:, :64]], axis=1),
        jnp.concatenate([first[:, 64:], second[:, 64:]], axis=1),
    )


def merge_kernel(
    mix, a_gate, b_gate, a_up, b_up, router, gain, merged, sums, inputs, row_sums, sems
):
    def copy(k, source, pair):
        return pltpu.make_async_copy(
            source.at[pl.ds(2 * pair, 2)], inputs.at[k, pl.ds(2 * pair, 2)], sems.at[k, pair]
        )

    sources = (a_gate, b_gate, a_up, b_up)
    for pair in range(PAIRS):
        for k, source in enumerate(sources):
            copy(k, source, pair).start()

    served = router[...] * gain[...]
    served = jnp.concatenate([served[:8], served[8:]], axis=1)
    for s in range(S):
        sums[s, 8:, :] = served
    sublane = lax.broadcasted_iota(jnp.int32, (8, 128), 0)

    def step(pair, carry):
        for t in range(2):
            for k in (2 * t, 2 * t + 1):
                copy(k, sources[k], pair).wait()
            for par in range(2):
                e = 2 * pair + par
                share = mix[e]
                other = 1.0 - share
                for j in range(C // 128):
                    cols = slice(j * 128, (j + 1) * 128)
                    m = share * inputs[2 * t, e, :, cols] + other * inputs[2 * t + 1, e, :, cols]
                    merged[t * E + e, :, cols] = m
                    row_sums[t * 2 + pair // 4, :, cols] = jnp.where(
                        sublane == e % 8,
                        jnp.sum(jnp.abs(m), axis=0, keepdims=True),
                        row_sums[t * 2 + pair // 4, :, cols],
                    )
        return carry

    lax.fori_loop(0, PAIRS, step, 0)
    for j in range(C // 128):
        tiles = regroup([row_sums[g, :, j * 128 : (j + 1) * 128] for g in range(4)])
        for dd in range(4):
            sums[PLACE[j * 4 + dd], :8, :] = tiles[dd]


def scale_kernel(parts, spread, router, scale_gate, scale_up):
    scale = jnp.sum(parts[:, :8, :], axis=0) / D_MODEL
    for k in range(S // 2):
        low, high = join(parts[PLACE[2 * k], 8:, :], parts[PLACE[2 * k + 1], 8:, :])
        router[:, k * 128 : (k + 1) * 128] = jnp.concatenate([low, high], axis=0).astype(
            jnp.bfloat16
        )
    for s in range(S):
        spread[s] = scale
    for g in range(4):
        out = scale_gate if g < 2 else scale_up
        out[(g % 2) * 8 : (g % 2) * 8 + 8, :] = scale[:, g * W : (g + 1) * W]


def pack_kernel(merged, scales, packed, inverse):
    for j in range(C // 128):
        tiles = regroup([scales[PLACE[4 * j + dd]] for dd in range(4)])
        for g in range(4):
            inverse[g, :, j * 128 : (j + 1) * 128] = 1.0 / tiles[g]

    for j in range(C // 128):
        cols = slice(j * 128, (j + 1) * 128)
        for tp in range(TP):
            halves = []
            for par in range(2):
                te = 2 * tp + par
                factor = inverse[te // 8, te % 8 : te % 8 + 1, cols]
                halves.append((merged[te, :, cols] * factor).astype(jnp.bfloat16))
            turned = jnp.concatenate(halves, axis=0).T
            for dd in range(4):
                rows = slice(tp * W, (tp + 1) * W)
                packed[PLACE[4 * j + dd], rows, :] = turned[dd * W : (dd + 1) * W]


def unpack_kernel(
    arrived, r0, r1, r2, r3, out_gate, out_up, out_router, joined, out_sems, router_sems
):
    me = lax.axis_index("expert")
    routers = (r0, r1, r2, r3)

    def serve(k):
        rows = pl.ds(pl.multiple_of(lax.rem(me + 4 - k, 4) * E, E), E)
        return pltpu.make_async_copy(routers[k], out_router.at[rows], router_sems.at[k])

    def give(t, p):
        out = (out_gate, out_up)[t]
        return pltpu.make_async_copy(
            joined.at[t, pl.ds(2 * p, 2)], out.at[pl.ds(2 * p, 2)], out_sems.at[t, p]
        )

    def step(p, carry):
        for t in range(2):
            rows = pl.ds(pl.multiple_of((t * PAIRS + p) * W, W), W)
            for k in range(S // 2):
                cols = slice(k * 128, (k + 1) * 128)
                even, odd = join(arrived[PLACE[2 * k], rows], arrived[PLACE[2 * k + 1], rows])
                joined[t, 2 * p, :, cols] = even
                joined[t, 2 * p + 1, :, cols] = odd
            give(t, p).start()
        return carry

    for k in range(4):
        serve(k).start()
    lax.fori_loop(0, PAIRS, step, 0)
    for p in range(PAIRS):
        for t in range(2):
            give(t, p).wait()
    for k in range(4):
        serve(k).wait()


def whole():
    return pl.BlockSpec(memory_space=pltpu.VMEM)


def remote():
    return pl.BlockSpec(memory_space=pltpu.HBM)


def params(mib):
    return pltpu.CompilerParams(vmem_limit_bytes=mib * MIB)


def exchange(x):
    return lax.all_to_all(
        x, "shard", split_axis=0, concat_axis=0, tiled=True, axis_index_groups=[ORDER]
    )


def serve_step(master_gate, second_gate, master_up, second_up, mix_share, router_weight, router_gain):
    merged, sums = pl.pallas_call(
        merge_kernel,
        in_specs=[pl.BlockSpec(memory_space=pltpu.SMEM)] + [remote()] * 4 + [whole()] * 2,
        out_specs=[whole(), whole()],
        out_shape=[
            pltpu.VMEM((2 * E, R, C), jnp.float32),
            pltpu.VMEM((S, 16, 128), jnp.float32),
        ],
        scratch_shapes=[
            pltpu.VMEM((4, E, R, C), jnp.float32),
            pltpu.VMEM((4, 8, C), jnp.float32),
            pltpu.SemaphoreType.DMA((4, PAIRS)),
        ],
        compiler_params=params(20),
        name="merge",
    )(
        *(
            pltpu.with_memory_space_constraint(x, pltpu.HBM)
            for x in (mix_share, master_gate, second_gate, master_up, second_up)
        ),
        pltpu.with_memory_space_constraint(router_weight.T, pltpu.HBM),
        pltpu.with_memory_space_constraint(router_gain[None, :], pltpu.HBM),
    )

    parts = exchange(sums)

    spread, router, scale_gate, scale_up = pl.pallas_call(
        scale_kernel,
        in_specs=[whole()],
        out_specs=[whole()] * 4,
        out_shape=[
            pltpu.VMEM((S, 8, 128), jnp.float32),
            pltpu.VMEM((E, S * R), jnp.bfloat16),
            jax.ShapeDtypeStruct((E, W), jnp.float32),
            jax.ShapeDtypeStruct((E, W), jnp.float32),
        ],
        compiler_params=params(4),
        name="scale",
    )(parts)
    hops = [
        lax.ppermute(router, "expert", [(z, (z + k) % 4) for z in range(4)])
        for k in range(1, 4)
    ]
    scales = exchange(spread)

    packed = pl.pallas_call(
        pack_kernel,
        in_specs=[whole()] * 2,
        out_specs=whole(),
        out_shape=pltpu.VMEM((S, TP * W, 128), jnp.bfloat16),
        scratch_shapes=[pltpu.VMEM((4, 8, C), jnp.float32)],
        compiler_params=params(4),
        name="pack",
    )(merged, scales)
    arrived = pltpu.with_memory_space_constraint(exchange(packed), pltpu.VMEM)

    final_gate, final_up, serve_router = pl.pallas_call(
        unpack_kernel,
        in_specs=[whole()] * 5,
        out_specs=[remote()] * 3,
        out_shape=[jax.ShapeDtypeStruct((E, W, S * R), jnp.bfloat16)] * 2
        + [jax.ShapeDtypeStruct((4 * E, S * R), jnp.bfloat16)],
        scratch_shapes=[
            pltpu.VMEM((2, E, W, S * R), jnp.bfloat16),
            pltpu.SemaphoreType.DMA((2, PAIRS)),
            pltpu.SemaphoreType.DMA((4,)),
        ],
        compiler_params=params(10),
        name="unpack",
    )(arrived, router, *hops)
    return (
        final_gate.transpose(0, 2, 1),
        final_up.transpose(0, 2, 1),
        scale_gate,
        scale_up,
        serve_router.T,
    )


def solution(mesh):
    in_specs = (
        P("expert", "shard", None),
        P("expert", "shard", None),
        P("expert", "shard", None),
        P("expert", "shard", None),
        P("expert"),
        P("shard", "expert"),
        P("shard"),
    )
    out_specs = (
        P("expert", None, "shard"),
        P("expert", None, "shard"),
        P("expert", "shard"),
        P("expert", "shard"),
        P(),
    )
    return jax.shard_map(serve_step, mesh=mesh, in_specs=in_specs, out_specs=out_specs, check_vma=False)
```

```python
import jax
import jax.numpy as jnp
from jax import lax
from jax.experimental import pallas as pl
from jax.experimental.pallas import tpu as pltpu
from jax.sharding import PartitionSpec as P


D_MODEL = 2048
E, R, C, S = 16, 64, 1024, 32
W = C // S
PAIRS = E // 2
TP = 2 * PAIRS
MIB = 1024 * 1024
ORDER = [13, 3, 31, 6, 26, 27, 11, 25, 4, 18, 9, 17, 30, 0, 16, 15, 7, 12, 24, 1, 5, 23, 22, 28, 10, 20, 19, 8, 2, 21, 14, 29]
PLACE = [ORDER.index(s) for s in range(S)]


def lanes(shape):
    return lax.broadcasted_iota(jnp.int32, shape, 1)


def regroup(blocks):
    group = lanes((8, 128)) // W
    out = []
    for a in range(4):
        tile = blocks[0]
        for b in range(4):
            shift = ((b - a) * W) % 128
            moved = pltpu.roll(blocks[b], shift, 1) if shift else blocks[b]
            tile = moved if b == 0 else jnp.where(group == b, moved, tile)
        out.append(tile)
    return out


def join(first, second):
    return (
        jnp.concatenate([first[:, :64], second[:, :64]], axis=1),
        jnp.concatenate([first[:, 64:], second[:, 64:]], axis=1),
    )


def merge_kernel(
    mix, a_gate, b_gate, a_up, b_up, router, gain, merged, sums, inputs, row_sums, sems
):
    def copy(k, source, pair):
        return pltpu.make_async_copy(
            source.at[pl.ds(2 * pair, 2)], inputs.at[k, pl.ds(2 * pair, 2)], sems.at[k, pair]
        )

    sources = (a_gate, b_gate, a_up, b_up)
    for pair in range(PAIRS):
        for k, source in enumerate(sources):
            copy(k, source, pair).start()

    served = router[...] * gain[...]
    served = jnp.concatenate([served[:8], served[8:]], axis=1).astype(jnp.bfloat16)
    for s in range(S):
        sums[s, 16:, :] = served
    sublane = lax.broadcasted_iota(jnp.int32, (8, 128), 0)

    def step(pair, carry):
        for t in range(2):
            for k in (2 * t, 2 * t + 1):
                copy(k, sources[k], pair).wait()
            for par in range(2):
                e = 2 * pair + par
                share = mix[e]
                other = 1.0 - share
                for j in range(C // 128):
                    cols = slice(j * 128, (j + 1) * 128)
                    m = share * inputs[2 * t, e, :, cols] + other * inputs[2 * t + 1, e, :, cols]
                    merged[t * E + e, :, cols] = m
                    row_sums[t * 2 + pair // 4, :, cols] = jnp.where(
                        sublane == e % 8,
                        jnp.sum(jnp.abs(m), axis=0, keepdims=True),
                        row_sums[t * 2 + pair // 4, :, cols],
                    )
        return carry

    lax.fori_loop(0, PAIRS, step, 0)
    for j in range(C // 128):
        tiles = regroup([row_sums[g, :, j * 128 : (j + 1) * 128] for g in range(4)])
        for dd in range(4):
            high = tiles[dd].astype(jnp.bfloat16)
            rest = (tiles[dd] - high.astype(jnp.float32)).astype(jnp.bfloat16)
            sums[PLACE[j * 4 + dd], :8, :] = high
            sums[PLACE[j * 4 + dd], 8:16, :] = rest


def scale_kernel(parts, spread, router, scale_gate, scale_up):
    both = parts[:, :8, :].astype(jnp.float32) + parts[:, 8:16, :].astype(jnp.float32)
    scale = jnp.sum(both, axis=0) / D_MODEL
    for k in range(S // 2):
        low, high = join(parts[PLACE[2 * k], 16:, :], parts[PLACE[2 * k + 1], 16:, :])
        router[:, k * 128 : (k + 1) * 128] = jnp.concatenate([low, high], axis=0)
    for s in range(S):
        spread[s] = scale
    for g in range(4):
        out = scale_gate if g < 2 else scale_up
        out[(g % 2) * 8 : (g % 2) * 8 + 8, :] = scale[:, g * W : (g + 1) * W]


def pack_kernel(merged, scales, packed, inverse):
    for j in range(C // 128):
        tiles = regroup([scales[PLACE[4 * j + dd]] for dd in range(4)])
        for g in range(4):
            inverse[g, :, j * 128 : (j + 1) * 128] = 1.0 / tiles[g]

    for j in range(C // 128):
        cols = slice(j * 128, (j + 1) * 128)
        for tp in range(TP):
            halves = []
            for par in range(2):
                te = 2 * tp + par
                factor = inverse[te // 8, te % 8 : te % 8 + 1, cols]
                halves.append((merged[te, :, cols] * factor).astype(jnp.bfloat16))
            turned = jnp.concatenate(halves, axis=0).T
            for dd in range(4):
                rows = slice(tp * W, (tp + 1) * W)
                packed[PLACE[4 * j + dd], rows, :] = turned[dd * W : (dd + 1) * W]


def unpack_kernel(
    arrived, r0, r1, r2, r3, out_gate, out_up, out_router, joined, out_sems, router_sems
):
    me = lax.axis_index("expert")
    routers = (r0, r1, r2, r3)

    def serve(k):
        rows = pl.ds(pl.multiple_of(lax.rem(me + 4 - k, 4) * E, E), E)
        return pltpu.make_async_copy(routers[k], out_router.at[rows], router_sems.at[k])

    def give(t, p):
        out = (out_gate, out_up)[t]
        return pltpu.make_async_copy(
            joined.at[t, pl.ds(2 * p, 2)], out.at[pl.ds(2 * p, 2)], out_sems.at[t, p]
        )

    def step(p, carry):
        for t in range(2):
            rows = pl.ds(pl.multiple_of((t * PAIRS + p) * W, W), W)
            for k in range(S // 2):
                cols = slice(k * 128, (k + 1) * 128)
                even, odd = join(arrived[PLACE[2 * k], rows], arrived[PLACE[2 * k + 1], rows])
                joined[t, 2 * p, :, cols] = even
                joined[t, 2 * p + 1, :, cols] = odd
            give(t, p).start()
        return carry

    for k in range(4):
        serve(k).start()
    lax.fori_loop(0, PAIRS, step, 0)
    for p in range(PAIRS):
        for t in range(2):
            give(t, p).wait()
    for k in range(4):
        serve(k).wait()


def whole():
    return pl.BlockSpec(memory_space=pltpu.VMEM)


def remote():
    return pl.BlockSpec(memory_space=pltpu.HBM)


def params(mib):
    return pltpu.CompilerParams(vmem_limit_bytes=mib * MIB)


def exchange(x):
    return lax.all_to_all(
        x, "shard", split_axis=0, concat_axis=0, tiled=True, axis_index_groups=[ORDER]
    )


def serve_step(master_gate, second_gate, master_up, second_up, mix_share, router_weight, router_gain):
    merged, sums = pl.pallas_call(
        merge_kernel,
        in_specs=[pl.BlockSpec(memory_space=pltpu.SMEM)] + [remote()] * 4 + [whole()] * 2,
        out_specs=[whole(), whole()],
        out_shape=[
            pltpu.VMEM((2 * E, R, C), jnp.float32),
            pltpu.VMEM((S, 24, 128), jnp.bfloat16),
        ],
        scratch_shapes=[
            pltpu.VMEM((4, E, R, C), jnp.float32),
            pltpu.VMEM((4, 8, C), jnp.float32),
            pltpu.SemaphoreType.DMA((4, PAIRS)),
        ],
        compiler_params=params(20),
        name="merge",
    )(
        *(
            pltpu.with_memory_space_constraint(x, pltpu.HBM)
            for x in (mix_share, master_gate, second_gate, master_up, second_up)
        ),
        pltpu.with_memory_space_constraint(router_weight.T, pltpu.HBM),
        pltpu.with_memory_space_constraint(router_gain[None, :], pltpu.HBM),
    )

    parts = exchange(sums)

    spread, router, scale_gate, scale_up = pl.pallas_call(
        scale_kernel,
        in_specs=[whole()],
        out_specs=[whole()] * 4,
        out_shape=[
            pltpu.VMEM((S, 8, 128), jnp.float32),
            pltpu.VMEM((E, S * R), jnp.bfloat16),
            jax.ShapeDtypeStruct((E, W), jnp.float32),
            jax.ShapeDtypeStruct((E, W), jnp.float32),
        ],
        compiler_params=params(4),
        name="scale",
    )(parts)
    hops = [
        lax.ppermute(router, "expert", [(z, (z + k) % 4) for z in range(4)])
        for k in range(1, 4)
    ]
    scales = exchange(spread)

    packed = pl.pallas_call(
        pack_kernel,
        in_specs=[whole()] * 2,
        out_specs=whole(),
        out_shape=pltpu.VMEM((S, TP * W, 128), jnp.bfloat16),
        scratch_shapes=[pltpu.VMEM((4, 8, C), jnp.float32)],
        compiler_params=params(4),
        name="pack",
    )(merged, scales)
    arrived = pltpu.with_memory_space_constraint(exchange(packed), pltpu.VMEM)

    final_gate, final_up, serve_router = pl.pallas_call(
        unpack_kernel,
        in_specs=[whole()] * 5,
        out_specs=[remote()] * 3,
        out_shape=[jax.ShapeDtypeStruct((E, W, S * R), jnp.bfloat16)] * 2
        + [jax.ShapeDtypeStruct((4 * E, S * R), jnp.bfloat16)],
        scratch_shapes=[
            pltpu.VMEM((2, E, W, S * R), jnp.bfloat16),
            pltpu.SemaphoreType.DMA((2, PAIRS)),
            pltpu.SemaphoreType.DMA((4,)),
        ],
        compiler_params=params(10),
        name="unpack",
    )(arrived, router, *hops)
    return (
        final_gate.transpose(0, 2, 1),
        final_up.transpose(0, 2, 1),
        scale_gate,
        scale_up,
        serve_router.T,
    )


def solution(mesh):
    in_specs = (
        P("expert", "shard", None),
        P("expert", "shard", None),
        P("expert", "shard", None),
        P("expert", "shard", None),
        P("expert"),
        P("shard", "expert"),
        P("shard"),
    )
    out_specs = (
        P("expert", None, "shard"),
        P("expert", None, "shard"),
        P("expert", "shard"),
        P("expert", "shard"),
        P(),
    )
    return jax.shard_map(serve_step, mesh=mesh, in_specs=in_specs, out_specs=out_specs, check_vma=False)
```

```python
import jax
import jax.numpy as jnp
from jax import lax
from jax.experimental import pallas as pl
from jax.experimental.pallas import tpu as pltpu
from jax.sharding import PartitionSpec as P


D_MODEL = 2048
E, R, C, S = 16, 64, 1024, 32
W = C // S
PAIRS = E // 2
TP = 2 * PAIRS
MIB = 1024 * 1024
ORDER = [13, 3, 31, 6, 26, 27, 11, 25, 4, 18, 9, 17, 30, 0, 16, 15, 7, 12, 24, 1, 5, 23, 22, 28, 10, 20, 19, 8, 2, 21, 14, 29]
PLACE = [ORDER.index(s) for s in range(S)]


def lanes(shape):
    return lax.broadcasted_iota(jnp.int32, shape, 1)


def regroup(blocks):
    group = lanes((8, 128)) // W
    out = []
    for a in range(4):
        tile = blocks[0]
        for b in range(4):
            shift = ((b - a) * W) % 128
            moved = pltpu.roll(blocks[b], shift, 1) if shift else blocks[b]
            tile = moved if b == 0 else jnp.where(group == b, moved, tile)
        out.append(tile)
    return out


def join(first, second):
    return (
        jnp.concatenate([first[:, :64], second[:, :64]], axis=1),
        jnp.concatenate([first[:, 64:], second[:, 64:]], axis=1),
    )


def merge_kernel(
    mix, a_gate, b_gate, a_up, b_up, router, gain, merged, sums, inputs, row_sums, sems
):
    def copy(k, source, pair):
        return pltpu.make_async_copy(
            source.at[pl.ds(2 * pair, 2)], inputs.at[k, pl.ds(2 * pair, 2)], sems.at[k, pair]
        )

    sources = (a_gate, b_gate, a_up, b_up)
    for pair in range(PAIRS):
        for k, source in enumerate(sources):
            copy(k, source, pair).start()

    served = router[...] * gain[...]
    served = jnp.concatenate([served[:8], served[8:]], axis=1).astype(jnp.bfloat16)
    for s in range(S):
        sums[s, 16:, :] = served
    sublane = lax.broadcasted_iota(jnp.int32, (8, 128), 0)

    def step(pair, carry):
        for t in range(2):
            for k in (2 * t, 2 * t + 1):
                copy(k, sources[k], pair).wait()
            for par in range(2):
                e = 2 * pair + par
                share = mix[e]
                other = 1.0 - share
                for j in range(C // 128):
                    cols = slice(j * 128, (j + 1) * 128)
                    m = share * inputs[2 * t, e, :, cols] + other * inputs[2 * t + 1, e, :, cols]
                    merged[t * E + e, :, cols] = m
                    row_sums[t * 2 + pair // 4, :, cols] = jnp.where(
                        sublane == e % 8,
                        jnp.sum(jnp.abs(m), axis=0, keepdims=True),
                        row_sums[t * 2 + pair // 4, :, cols],
                    )
        return carry

    lax.fori_loop(0, PAIRS, step, 0)
    for j in range(C // 128):
        tiles = regroup([row_sums[g, :, j * 128 : (j + 1) * 128] for g in range(4)])
        for dd in range(4):
            high = tiles[dd].astype(jnp.bfloat16)
            rest = (tiles[dd] - high.astype(jnp.float32)).astype(jnp.bfloat16)
            sums[PLACE[j * 4 + dd], :8, :] = high
            sums[PLACE[j * 4 + dd], 8:16, :] = rest


def scale_kernel(parts, spread, router):
    both = parts[:, :8, :].astype(jnp.float32) + parts[:, 8:16, :].astype(jnp.float32)
    scale = jnp.sum(both, axis=0) / D_MODEL
    for k in range(S // 2):
        low, high = join(parts[PLACE[2 * k], 16:, :], parts[PLACE[2 * k + 1], 16:, :])
        router[:, k * 128 : (k + 1) * 128] = jnp.concatenate([low, high], axis=0)
    for s in range(S):
        spread[s] = scale


def pack_kernel(merged, scales, packed, inverse):
    for j in range(C // 128):
        tiles = regroup([scales[PLACE[4 * j + dd]] for dd in range(4)])
        for g in range(4):
            inverse[g, :, j * 128 : (j + 1) * 128] = 1.0 / tiles[g]

    for j in range(C // 128):
        cols = slice(j * 128, (j + 1) * 128)
        for tp in range(TP):
            halves = []
            for par in range(2):
                te = 2 * tp + par
                factor = inverse[te // 8, te % 8 : te % 8 + 1, cols]
                halves.append((merged[te, :, cols] * factor).astype(jnp.bfloat16))
            turned = jnp.concatenate(halves, axis=0).T
            for dd in range(4):
                rows = slice(tp * W, (tp + 1) * W)
                packed[PLACE[4 * j + dd], rows, :] = turned[dd * W : (dd + 1) * W]


def unpack_kernel(
    arrived, spread, r0, r1, r2, r3, out_gate, out_up, out_router, scale_gate, scale_up, *scratch
):
    joined, scales, out_sems, router_sems, scale_sems = scratch
    me = lax.axis_index("expert")
    routers = (r0, r1, r2, r3)

    def serve(k):
        rows = pl.ds(pl.multiple_of(lax.rem(me + 4 - k, 4) * E, E), E)
        return pltpu.make_async_copy(routers[k], out_router.at[rows], router_sems.at[k])

    def give(t, p):
        out = (out_gate, out_up)[t]
        return pltpu.make_async_copy(
            joined.at[t, pl.ds(2 * p, 2)], out.at[pl.ds(2 * p, 2)], out_sems.at[t, p]
        )

    def step(p, carry):
        for t in range(2):
            rows = pl.ds(pl.multiple_of((t * PAIRS + p) * W, W), W)
            for k in range(S // 2):
                cols = slice(k * 128, (k + 1) * 128)
                even, odd = join(arrived[PLACE[2 * k], rows], arrived[PLACE[2 * k + 1], rows])
                joined[t, 2 * p, :, cols] = even
                joined[t, 2 * p + 1, :, cols] = odd
            give(t, p).start()
        return carry

    for k in range(4):
        serve(k).start()
    for g in range(4):
        rows = slice((g % 2) * 8, (g % 2) * 8 + 8)
        scales[g // 2, rows, :] = spread[0, :, g * W : (g + 1) * W]
    scaled = [
        pltpu.make_async_copy(scales.at[t], out, scale_sems.at[t])
        for t, out in enumerate((scale_gate, scale_up))
    ]
    for each in scaled:
        each.start()
    lax.fori_loop(0, PAIRS, step, 0)
    for p in range(PAIRS):
        for t in range(2):
            give(t, p).wait()
    for k in range(4):
        serve(k).wait()
    for each in scaled:
        each.wait()


def whole():
    return pl.BlockSpec(memory_space=pltpu.VMEM)


def remote():
    return pl.BlockSpec(memory_space=pltpu.HBM)


def params(mib):
    return pltpu.CompilerParams(vmem_limit_bytes=mib * MIB)


def exchange(x):
    return lax.all_to_all(
        x, "shard", split_axis=0, concat_axis=0, tiled=True, axis_index_groups=[ORDER]
    )


def serve_step(master_gate, second_gate, master_up, second_up, mix_share, router_weight, router_gain):
    merged, sums = pl.pallas_call(
        merge_kernel,
        in_specs=[pl.BlockSpec(memory_space=pltpu.SMEM)] + [remote()] * 4 + [whole()] * 2,
        out_specs=[whole(), whole()],
        out_shape=[
            pltpu.VMEM((2 * E, R, C), jnp.float32),
            pltpu.VMEM((S, 24, 128), jnp.bfloat16),
        ],
        scratch_shapes=[
            pltpu.VMEM((4, E, R, C), jnp.float32),
            pltpu.VMEM((4, 8, C), jnp.float32),
            pltpu.SemaphoreType.DMA((4, PAIRS)),
        ],
        compiler_params=params(20),
        name="merge",
    )(
        *(
            pltpu.with_memory_space_constraint(x, pltpu.HBM)
            for x in (mix_share, master_gate, second_gate, master_up, second_up)
        ),
        pltpu.with_memory_space_constraint(router_weight.T, pltpu.HBM),
        pltpu.with_memory_space_constraint(router_gain[None, :], pltpu.HBM),
    )

    parts = exchange(sums)

    spread, router = pl.pallas_call(
        scale_kernel,
        in_specs=[whole()],
        out_specs=[whole()] * 2,
        out_shape=[
            pltpu.VMEM((S, 8, 128), jnp.float32),
            pltpu.VMEM((E, S * R), jnp.bfloat16),
        ],
        compiler_params=params(4),
        name="scale",
    )(parts)
    hops = [
        lax.ppermute(router, "expert", [(z, (z + k) % 4) for z in range(4)])
        for k in range(1, 4)
    ]
    scales = exchange(spread)

    packed = pl.pallas_call(
        pack_kernel,
        in_specs=[whole()] * 2,
        out_specs=whole(),
        out_shape=pltpu.VMEM((S, TP * W, 128), jnp.bfloat16),
        scratch_shapes=[pltpu.VMEM((4, 8, C), jnp.float32)],
        compiler_params=params(4),
        name="pack",
    )(merged, scales)
    arrived = pltpu.with_memory_space_constraint(exchange(packed), pltpu.VMEM)

    final_gate, final_up, serve_router, scale_gate, scale_up = pl.pallas_call(
        unpack_kernel,
        in_specs=[whole()] * 6,
        out_specs=[remote()] * 5,
        out_shape=[jax.ShapeDtypeStruct((E, W, S * R), jnp.bfloat16)] * 2
        + [jax.ShapeDtypeStruct((4 * E, S * R), jnp.bfloat16)]
        + [jax.ShapeDtypeStruct((E, W), jnp.float32)] * 2,
        scratch_shapes=[
            pltpu.VMEM((2, E, W, S * R), jnp.bfloat16),
            pltpu.VMEM((2, E, W), jnp.float32),
            pltpu.SemaphoreType.DMA((2, PAIRS)),
            pltpu.SemaphoreType.DMA((4,)),
            pltpu.SemaphoreType.DMA((2,)),
        ],
        compiler_params=params(10),
        name="unpack",
    )(arrived, spread, router, *hops)
    return (
        final_gate.transpose(0, 2, 1),
        final_up.transpose(0, 2, 1),
        scale_gate,
        scale_up,
        serve_router.T,
    )


def solution(mesh):
    in_specs = (
        P("expert", "shard", None),
        P("expert", "shard", None),
        P("expert", "shard", None),
        P("expert", "shard", None),
        P("expert"),
        P("shard", "expert"),
        P("shard"),
    )
    out_specs = (
        P("expert", None, "shard"),
        P("expert", None, "shard"),
        P("expert", "shard"),
        P("expert", "shard"),
        P(),
    )
    return jax.shard_map(serve_step, mesh=mesh, in_specs=in_specs, out_specs=out_specs, check_vma=False)
```

```python
import jax
import jax.numpy as jnp
from jax import lax
from jax.experimental import pallas as pl
from jax.experimental.pallas import tpu as pltpu
from jax.sharding import PartitionSpec as P


D_MODEL = 2048
E, R, C, S = 16, 64, 1024, 32
W = C // S
PAIRS = E // 2
TP = 2 * PAIRS
MIB = 1024 * 1024
ORDER = [13, 3, 31, 6, 26, 27, 11, 25, 4, 18, 9, 17, 30, 0, 16, 15, 7, 12, 24, 1, 5, 23, 22, 28, 10, 20, 19, 8, 2, 21, 14, 29]
PLACE = [ORDER.index(s) for s in range(S)]


def lanes(shape):
    return lax.broadcasted_iota(jnp.int32, shape, 1)


def regroup(blocks):
    group = lanes((8, 128)) // W
    out = []
    for a in range(4):
        tile = blocks[0]
        for b in range(4):
            shift = ((b - a) * W) % 128
            moved = pltpu.roll(blocks[b], shift, 1) if shift else blocks[b]
            tile = moved if b == 0 else jnp.where(group == b, moved, tile)
        out.append(tile)
    return out


def join(first, second):
    return (
        jnp.concatenate([first[:, :64], second[:, :64]], axis=1),
        jnp.concatenate([first[:, 64:], second[:, 64:]], axis=1),
    )


def merge_kernel(
    shares, a_gate, b_gate, a_up, b_up, weight, gains, merged, sums, *scratch
):
    inputs, row_sums, mix, router, gain, sems, small_sems = scratch

    def copy(k, source, pair):
        return pltpu.make_async_copy(
            source.at[pl.ds(2 * pair, 2)], inputs.at[k, pl.ds(2 * pair, 2)], sems.at[k, pair]
        )

    small = [
        pltpu.make_async_copy(source, target, small_sems.at[k])
        for k, (source, target) in enumerate(((shares, mix), (weight, router), (gains, gain)))
    ]
    for each in small:
        each.start()
    sources = (a_gate, b_gate, a_up, b_up)
    for pair in range(PAIRS):
        for k, source in enumerate(sources):
            copy(k, source, pair).start()
    small[0].wait()
    sublane = lax.broadcasted_iota(jnp.int32, (8, 128), 0)

    def step(pair, carry):
        for t in range(2):
            for k in (2 * t, 2 * t + 1):
                copy(k, sources[k], pair).wait()
            for par in range(2):
                e = 2 * pair + par
                share = mix[e]
                other = 1.0 - share
                for j in range(C // 128):
                    cols = slice(j * 128, (j + 1) * 128)
                    m = share * inputs[2 * t, e, :, cols] + other * inputs[2 * t + 1, e, :, cols]
                    merged[t * E + e, :, cols] = m
                    row_sums[t * 2 + pair // 4, :, cols] = jnp.where(
                        sublane == e % 8,
                        jnp.sum(jnp.abs(m), axis=0, keepdims=True),
                        row_sums[t * 2 + pair // 4, :, cols],
                    )
        return carry

    lax.fori_loop(0, PAIRS, step, 0)
    for each in small[1:]:
        each.wait()

    served = router[...] * gain[...]
    served = jnp.concatenate([served[:8], served[8:]], axis=1).astype(jnp.bfloat16)
    for s in range(S):
        sums[s, 16:, :] = served
    for j in range(C // 128):
        tiles = regroup([row_sums[g, :, j * 128 : (j + 1) * 128] for g in range(4)])
        for dd in range(4):
            high = tiles[dd].astype(jnp.bfloat16)
            rest = (tiles[dd] - high.astype(jnp.float32)).astype(jnp.bfloat16)
            sums[PLACE[j * 4 + dd], :8, :] = high
            sums[PLACE[j * 4 + dd], 8:16, :] = rest


def scale_kernel(parts, spread, router):
    both = parts[:, :8, :].astype(jnp.float32) + parts[:, 8:16, :].astype(jnp.float32)
    scale = jnp.sum(both, axis=0) / D_MODEL
    for k in range(S // 2):
        low, high = join(parts[PLACE[2 * k], 16:, :], parts[PLACE[2 * k + 1], 16:, :])
        router[:, k * 128 : (k + 1) * 128] = jnp.concatenate([low, high], axis=0)
    for s in range(S):
        spread[s] = scale


def pack_kernel(merged, scales, packed, inverse):
    for j in range(C // 128):
        tiles = regroup([scales[PLACE[4 * j + dd]] for dd in range(4)])
        for g in range(4):
            inverse[g, :, j * 128 : (j + 1) * 128] = 1.0 / tiles[g]

    for j in range(C // 128):
        cols = slice(j * 128, (j + 1) * 128)
        for tp in range(TP):
            halves = []
            for par in range(2):
                te = 2 * tp + par
                factor = inverse[te // 8, te % 8 : te % 8 + 1, cols]
                halves.append((merged[te, :, cols] * factor).astype(jnp.bfloat16))
            turned = jnp.concatenate(halves, axis=0).T
            for dd in range(4):
                rows = slice(tp * W, (tp + 1) * W)
                packed[PLACE[4 * j + dd], rows, :] = turned[dd * W : (dd + 1) * W]


def unpack_kernel(
    arrived, spread, r0, r1, r2, r3, out_gate, out_up, out_router, scale_gate, scale_up, *scratch
):
    joined, scales, out_sems, router_sems, scale_sems = scratch
    me = lax.axis_index("expert")
    routers = (r0, r1, r2, r3)

    def serve(k):
        rows = pl.ds(pl.multiple_of(lax.rem(me + 4 - k, 4) * E, E), E)
        return pltpu.make_async_copy(routers[k], out_router.at[rows], router_sems.at[k])

    def give(t, p):
        out = (out_gate, out_up)[t]
        return pltpu.make_async_copy(
            joined.at[t, pl.ds(2 * p, 2)], out.at[pl.ds(2 * p, 2)], out_sems.at[t, p]
        )

    def step(p, carry):
        for t in range(2):
            rows = pl.ds(pl.multiple_of((t * PAIRS + p) * W, W), W)
            for k in range(S // 2):
                cols = slice(k * 128, (k + 1) * 128)
                even, odd = join(arrived[PLACE[2 * k], rows], arrived[PLACE[2 * k + 1], rows])
                joined[t, 2 * p, :, cols] = even
                joined[t, 2 * p + 1, :, cols] = odd
            give(t, p).start()
        return carry

    for k in range(4):
        serve(k).start()
    for g in range(4):
        rows = slice((g % 2) * 8, (g % 2) * 8 + 8)
        scales[g // 2, rows, :] = spread[0, :, g * W : (g + 1) * W]
    scaled = [
        pltpu.make_async_copy(scales.at[t], out, scale_sems.at[t])
        for t, out in enumerate((scale_gate, scale_up))
    ]
    for each in scaled:
        each.start()
    lax.fori_loop(0, PAIRS, step, 0)
    for p in range(PAIRS):
        for t in range(2):
            give(t, p).wait()
    for k in range(4):
        serve(k).wait()
    for each in scaled:
        each.wait()


def whole():
    return pl.BlockSpec(memory_space=pltpu.VMEM)


def remote():
    return pl.BlockSpec(memory_space=pltpu.HBM)


def params(mib):
    return pltpu.CompilerParams(vmem_limit_bytes=mib * MIB)


def exchange(x):
    return lax.all_to_all(
        x, "shard", split_axis=0, concat_axis=0, tiled=True, axis_index_groups=[ORDER]
    )


def serve_step(master_gate, second_gate, master_up, second_up, mix_share, router_weight, router_gain):
    merged, sums = pl.pallas_call(
        merge_kernel,
        in_specs=[remote()] * 7,
        out_specs=[whole(), whole()],
        out_shape=[
            pltpu.VMEM((2 * E, R, C), jnp.float32),
            pltpu.VMEM((S, 24, 128), jnp.bfloat16),
        ],
        scratch_shapes=[
            pltpu.VMEM((4, E, R, C), jnp.float32),
            pltpu.VMEM((4, 8, C), jnp.float32),
            pltpu.SMEM((E,), jnp.float32),
            pltpu.VMEM((E, R), jnp.float32),
            pltpu.VMEM((1, R), jnp.float32),
            pltpu.SemaphoreType.DMA((4, PAIRS)),
            pltpu.SemaphoreType.DMA((3,)),
        ],
        compiler_params=params(20),
        name="merge",
    )(
        *(
            pltpu.with_memory_space_constraint(x, pltpu.HBM)
            for x in (mix_share, master_gate, second_gate, master_up, second_up)
        ),
        pltpu.with_memory_space_constraint(router_weight.T, pltpu.HBM),
        pltpu.with_memory_space_constraint(router_gain[None, :], pltpu.HBM),
    )

    parts = exchange(sums)

    spread, router = pl.pallas_call(
        scale_kernel,
        in_specs=[whole()],
        out_specs=[whole()] * 2,
        out_shape=[
            pltpu.VMEM((S, 8, 128), jnp.float32),
            pltpu.VMEM((E, S * R), jnp.bfloat16),
        ],
        compiler_params=params(4),
        name="scale",
    )(parts)
    hops = [
        lax.ppermute(router, "expert", [(z, (z + k) % 4) for z in range(4)])
        for k in range(1, 4)
    ]
    scales = exchange(spread)

    packed = pl.pallas_call(
        pack_kernel,
        in_specs=[whole()] * 2,
        out_specs=whole(),
        out_shape=pltpu.VMEM((S, TP * W, 128), jnp.bfloat16),
        scratch_shapes=[pltpu.VMEM((4, 8, C), jnp.float32)],
        compiler_params=params(4),
        name="pack",
    )(merged, scales)
    arrived = pltpu.with_memory_space_constraint(exchange(packed), pltpu.VMEM)

    final_gate, final_up, serve_router, scale_gate, scale_up = pl.pallas_call(
        unpack_kernel,
        in_specs=[whole()] * 6,
        out_specs=[remote()] * 5,
        out_shape=[jax.ShapeDtypeStruct((E, W, S * R), jnp.bfloat16)] * 2
        + [jax.ShapeDtypeStruct((4 * E, S * R), jnp.bfloat16)]
        + [jax.ShapeDtypeStruct((E, W), jnp.float32)] * 2,
        scratch_shapes=[
            pltpu.VMEM((2, E, W, S * R), jnp.bfloat16),
            pltpu.VMEM((2, E, W), jnp.float32),
            pltpu.SemaphoreType.DMA((2, PAIRS)),
            pltpu.SemaphoreType.DMA((4,)),
            pltpu.SemaphoreType.DMA((2,)),
        ],
        compiler_params=params(10),
        name="unpack",
    )(arrived, spread, router, *hops)
    return (
        final_gate.transpose(0, 2, 1),
        final_up.transpose(0, 2, 1),
        scale_gate,
        scale_up,
        serve_router.T,
    )


def solution(mesh):
    in_specs = (
        P("expert", "shard", None),
        P("expert", "shard", None),
        P("expert", "shard", None),
        P("expert", "shard", None),
        P("expert"),
        P("shard", "expert"),
        P("shard"),
    )
    out_specs = (
        P("expert", None, "shard"),
        P("expert", None, "shard"),
        P("expert", "shard"),
        P("expert", "shard"),
        P(),
    )
    return jax.shard_map(serve_step, mesh=mesh, in_specs=in_specs, out_specs=out_specs, check_vma=False)
```

```python
import jax
import jax.numpy as jnp
from jax import lax
from jax.experimental import pallas as pl
from jax.experimental.pallas import tpu as pltpu
from jax.sharding import PartitionSpec as P


D_MODEL = 2048
E, R, C, S = 16, 64, 1024, 32
W = C // S
PAIRS = E // 2
TP = 2 * PAIRS
MIB = 1024 * 1024
ORDER = [13, 3, 31, 6, 26, 27, 11, 25, 4, 18, 9, 17, 30, 0, 16, 15, 7, 12, 24, 1, 5, 23, 22, 28, 10, 20, 19, 8, 2, 21, 14, 29]
PLACE = [ORDER.index(s) for s in range(S)]


def lanes(shape):
    return lax.broadcasted_iota(jnp.int32, shape, 1)


def regroup(blocks):
    group = lanes((8, 128)) // W
    out = []
    for a in range(4):
        tile = blocks[0]
        for b in range(4):
            shift = ((b - a) * W) % 128
            moved = pltpu.roll(blocks[b], shift, 1) if shift else blocks[b]
            tile = moved if b == 0 else jnp.where(group == b, moved, tile)
        out.append(tile)
    return out


def join(first, second):
    return (
        jnp.concatenate([first[:, :64], second[:, :64]], axis=1),
        jnp.concatenate([first[:, 64:], second[:, 64:]], axis=1),
    )


def merge_kernel(
    shares, a_gate, b_gate, a_up, b_up, weight, gains, merged, sums, *scratch
):
    inputs, row_sums, mix, router, gain, sems, small_sems = scratch

    def copy(k, source, pair):
        return pltpu.make_async_copy(
            source.at[pl.ds(2 * pair, 2)], inputs.at[k, pl.ds(2 * pair, 2)], sems.at[k, pair]
        )

    small = [
        pltpu.make_async_copy(source, target, small_sems.at[k])
        for k, (source, target) in enumerate(((shares, mix), (weight, router), (gains, gain)))
    ]
    for each in small:
        each.start()
    sources = (a_gate, b_gate, a_up, b_up)
    for pair in range(PAIRS):
        for k, source in enumerate(sources):
            copy(k, source, pair).start()
    small[0].wait()
    sublane = lax.broadcasted_iota(jnp.int32, (8, 128), 0)

    def step(pair, carry):
        for t in range(2):
            for k in (2 * t, 2 * t + 1):
                copy(k, sources[k], pair).wait()
            for par in range(2):
                e = 2 * pair + par
                share = mix[e]
                other = 1.0 - share
                for j in range(C // 128):
                    cols = slice(j * 128, (j + 1) * 128)
                    m = share * inputs[2 * t, e, :, cols] + other * inputs[2 * t + 1, e, :, cols]
                    merged[t * E + e, :, cols] = m
                    row_sums[t * 2 + pair // 4, :, cols] = jnp.where(
                        sublane == e % 8,
                        jnp.sum(jnp.abs(m), axis=0, keepdims=True),
                        row_sums[t * 2 + pair // 4, :, cols],
                    )
        return carry

    lax.fori_loop(0, PAIRS, step, 0)
    for each in small[1:]:
        each.wait()

    served = router[...] * gain[...]
    served = jnp.concatenate([served[:8], served[8:]], axis=1).astype(jnp.bfloat16)
    for s in range(S):
        sums[s, 16:, :] = served
    for j in range(C // 128):
        tiles = regroup([row_sums[g, :, j * 128 : (j + 1) * 128] for g in range(4)])
        for dd in range(4):
            high = tiles[dd].astype(jnp.bfloat16)
            rest = (tiles[dd] - high.astype(jnp.float32)).astype(jnp.bfloat16)
            sums[PLACE[j * 4 + dd], :8, :] = high
            sums[PLACE[j * 4 + dd], 8:16, :] = rest


def scale_kernel(parts, spread, router):
    both = parts[:, :8, :].astype(jnp.float32) + parts[:, 8:16, :].astype(jnp.float32)
    scale = jnp.sum(both, axis=0) / D_MODEL
    for k in range(S // 2):
        low, high = join(parts[PLACE[2 * k], 16:, :], parts[PLACE[2 * k + 1], 16:, :])
        router[:, k * 128 : (k + 1) * 128] = jnp.concatenate([low, high], axis=0)
    for s in range(S):
        spread[s] = scale


def pack_kernel(merged, scales, packed, inverse):
    for j in range(C // 128):
        tiles = regroup([scales[PLACE[4 * j + dd]] for dd in range(4)])
        for g in range(4):
            inverse[g, :, j * 128 : (j + 1) * 128] = 1.0 / tiles[g]

    for j in range(C // 128):
        cols = slice(j * 128, (j + 1) * 128)
        for tp in range(TP):
            halves = []
            for par in range(2):
                te = 2 * tp + par
                factor = inverse[te // 8, te % 8 : te % 8 + 1, cols]
                halves.append((merged[te, :, cols] * factor).astype(jnp.bfloat16))
            turned = jnp.concatenate(halves, axis=0).T
            for dd in range(4):
                rows = slice(tp * W, (tp + 1) * W)
                packed[PLACE[4 * j + dd], rows, :] = turned[dd * W : (dd + 1) * W]


def unpack_kernel(
    arrived, spread, r0, r1, r2, r3, out_gate, out_up, out_router, scale_gate, scale_up, *scratch
):
    joined, scales, out_sems, router_sems, scale_sems = scratch
    me = lax.axis_index("expert")
    routers = (r0, r1, r2, r3)

    def serve(k):
        rows = pl.ds(pl.multiple_of(lax.bitwise_xor(me, (0, 3, 2, 1)[k]) * E, E), E)
        return pltpu.make_async_copy(routers[k], out_router.at[rows], router_sems.at[k])

    def give(t, p):
        out = (out_gate, out_up)[t]
        return pltpu.make_async_copy(
            joined.at[t, pl.ds(2 * p, 2)], out.at[pl.ds(2 * p, 2)], out_sems.at[t, p]
        )

    def step(p, carry):
        for t in range(2):
            rows = slice((t * PAIRS + p) * W, (t * PAIRS + p + 1) * W)
            for k in range(S // 2):
                cols = slice(k * 128, (k + 1) * 128)
                even, odd = join(arrived[PLACE[2 * k], rows], arrived[PLACE[2 * k + 1], rows])
                joined[t, 2 * p, :, cols] = even
                joined[t, 2 * p + 1, :, cols] = odd
            give(t, p).start()
        return carry

    for k in range(4):
        serve(k).start()
    for g in range(4):
        rows = slice((g % 2) * 8, (g % 2) * 8 + 8)
        scales[g // 2, rows, :] = spread[0, :, g * W : (g + 1) * W]
    scaled = [
        pltpu.make_async_copy(scales.at[t], out, scale_sems.at[t])
        for t, out in enumerate((scale_gate, scale_up))
    ]
    for each in scaled:
        each.start()
    for p in range(PAIRS):
        step(p, 0)
    for p in range(PAIRS):
        for t in range(2):
            give(t, p).wait()
    for k in range(4):
        serve(k).wait()
    for each in scaled:
        each.wait()


def whole():
    return pl.BlockSpec(memory_space=pltpu.VMEM)


def remote():
    return pl.BlockSpec(memory_space=pltpu.HBM)


def params(mib):
    return pltpu.CompilerParams(vmem_limit_bytes=mib * MIB)


def exchange(x):
    return lax.all_to_all(
        x, "shard", split_axis=0, concat_axis=0, tiled=True, axis_index_groups=[ORDER]
    )


def serve_step(master_gate, second_gate, master_up, second_up, mix_share, router_weight, router_gain):
    merged, sums = pl.pallas_call(
        merge_kernel,
        in_specs=[remote()] * 7,
        out_specs=[whole(), whole()],
        out_shape=[
            pltpu.VMEM((2 * E, R, C), jnp.float32),
            pltpu.VMEM((S, 24, 128), jnp.bfloat16),
        ],
        scratch_shapes=[
            pltpu.VMEM((4, E, R, C), jnp.float32),
            pltpu.VMEM((4, 8, C), jnp.float32),
            pltpu.SMEM((E,), jnp.float32),
            pltpu.VMEM((E, R), jnp.float32),
            pltpu.VMEM((1, R), jnp.float32),
            pltpu.SemaphoreType.DMA((4, PAIRS)),
            pltpu.SemaphoreType.DMA((3,)),
        ],
        compiler_params=params(20),
        name="merge",
    )(
        *(
            pltpu.with_memory_space_constraint(x, pltpu.HBM)
            for x in (mix_share, master_gate, second_gate, master_up, second_up)
        ),
        pltpu.with_memory_space_constraint(router_weight.T, pltpu.HBM),
        pltpu.with_memory_space_constraint(router_gain[None, :], pltpu.HBM),
    )

    parts = exchange(sums)

    spread, router = pl.pallas_call(
        scale_kernel,
        in_specs=[whole()],
        out_specs=[whole()] * 2,
        out_shape=[
            pltpu.VMEM((S, 8, 128), jnp.float32),
            pltpu.VMEM((E, S * R), jnp.bfloat16),
        ],
        compiler_params=params(4),
        name="scale",
    )(parts)
    hops = [
        lax.ppermute(router, "expert", [(z, z ^ k) for z in range(4)])
        for k in (3, 2, 1)
    ]
    scales = exchange(spread)

    packed = pl.pallas_call(
        pack_kernel,
        in_specs=[whole()] * 2,
        out_specs=whole(),
        out_shape=pltpu.VMEM((S, TP * W, 128), jnp.bfloat16),
        scratch_shapes=[pltpu.VMEM((4, 8, C), jnp.float32)],
        compiler_params=params(4),
        name="pack",
    )(merged, scales)
    arrived = pltpu.with_memory_space_constraint(exchange(packed), pltpu.VMEM)

    final_gate, final_up, serve_router, scale_gate, scale_up = pl.pallas_call(
        unpack_kernel,
        in_specs=[whole()] * 6,
        out_specs=[remote()] * 5,
        out_shape=[jax.ShapeDtypeStruct((E, W, S * R), jnp.bfloat16)] * 2
        + [jax.ShapeDtypeStruct((4 * E, S * R), jnp.bfloat16)]
        + [jax.ShapeDtypeStruct((E, W), jnp.float32)] * 2,
        scratch_shapes=[
            pltpu.VMEM((2, E, W, S * R), jnp.bfloat16),
            pltpu.VMEM((2, E, W), jnp.float32),
            pltpu.SemaphoreType.DMA((2, PAIRS)),
            pltpu.SemaphoreType.DMA((4,)),
            pltpu.SemaphoreType.DMA((2,)),
        ],
        compiler_params=params(10),
        name="unpack",
    )(arrived, spread, router, *hops)
    return (
        final_gate.transpose(0, 2, 1),
        final_up.transpose(0, 2, 1),
        scale_gate,
        scale_up,
        serve_router.T,
    )


def solution(mesh):
    in_specs = (
        P("expert", "shard", None),
        P("expert", "shard", None),
        P("expert", "shard", None),
        P("expert", "shard", None),
        P("expert"),
        P("shard", "expert"),
        P("shard"),
    )
    out_specs = (
        P("expert", None, "shard"),
        P("expert", None, "shard"),
        P("expert", "shard"),
        P("expert", "shard"),
        P(),
    )
    return jax.shard_map(serve_step, mesh=mesh, in_specs=in_specs, out_specs=out_specs, check_vma=False)
```

```python
import jax
import jax.numpy as jnp
from jax import lax
from jax.experimental import pallas as pl
from jax.experimental.pallas import tpu as pltpu
from jax.sharding import PartitionSpec as P


D_MODEL = 2048
E, R, C, S = 16, 64, 1024, 32
W = C // S
PAIRS = E // 2
TP = 2 * PAIRS
MIB = 1024 * 1024
ORDER = [13, 3, 31, 6, 26, 27, 11, 25, 4, 18, 9, 17, 30, 0, 16, 15, 7, 12, 24, 1, 5, 23, 22, 28, 10, 20, 19, 8, 2, 21, 14, 29]
PLACE = [ORDER.index(s) for s in range(S)]


def lanes(shape):
    return lax.broadcasted_iota(jnp.int32, shape, 1)


def regroup(blocks):
    group = lanes((8, 128)) // W
    out = []
    for a in range(4):
        tile = blocks[0]
        for b in range(4):
            shift = ((b - a) * W) % 128
            moved = pltpu.roll(blocks[b], shift, 1) if shift else blocks[b]
            tile = moved if b == 0 else jnp.where(group == b, moved, tile)
        out.append(tile)
    return out


def join(first, second):
    return (
        jnp.concatenate([first[:, :64], second[:, :64]], axis=1),
        jnp.concatenate([first[:, 64:], second[:, 64:]], axis=1),
    )


def merge_kernel(
    shares, a_gate, b_gate, a_up, b_up, weight, gains, merged, sums, *scratch
):
    inputs, row_sums, mix, router, gain, sems, small_sems = scratch

    def copy(k, source, pair):
        return pltpu.make_async_copy(
            source.at[pl.ds(2 * pair, 2)], inputs.at[k, pl.ds(2 * pair, 2)], sems.at[k, pair]
        )

    small = [
        pltpu.make_async_copy(source, target, small_sems.at[k])
        for k, (source, target) in enumerate(((shares, mix), (weight, router), (gains, gain)))
    ]
    for each in small:
        each.start()
    sources = (a_gate, b_gate, a_up, b_up)
    for pair in range(PAIRS):
        for k, source in enumerate(sources):
            copy(k, source, pair).start()
    small[0].wait()
    sublane = lax.broadcasted_iota(jnp.int32, (8, 128), 0)

    def step(pair, carry):
        for t in range(2):
            for k in (2 * t, 2 * t + 1):
                copy(k, sources[k], pair).wait()
            for par in range(2):
                e = 2 * pair + par
                share = mix[e]
                other = 1.0 - share
                for j in range(C // 128):
                    cols = slice(j * 128, (j + 1) * 128)
                    m = share * inputs[2 * t, e, :, cols] + other * inputs[2 * t + 1, e, :, cols]
                    merged[t * E + e, :, cols] = m
                    row_sums[t * 2 + pair // 4, :, cols] = jnp.where(
                        sublane == e % 8,
                        jnp.sum(jnp.abs(m), axis=0, keepdims=True),
                        row_sums[t * 2 + pair // 4, :, cols],
                    )
        return carry

    lax.fori_loop(0, PAIRS, step, 0)
    for each in small[1:]:
        each.wait()

    served = router[...] * gain[...]
    served = jnp.concatenate([served[:8], served[8:]], axis=1).astype(jnp.bfloat16)
    for s in range(S):
        sums[s, 16:, :] = served
    for j in range(C // 128):
        tiles = regroup([row_sums[g, :, j * 128 : (j + 1) * 128] for g in range(4)])
        for dd in range(4):
            high = tiles[dd].astype(jnp.bfloat16)
            rest = (tiles[dd] - high.astype(jnp.float32)).astype(jnp.bfloat16)
            sums[PLACE[j * 4 + dd], :8, :] = high
            sums[PLACE[j * 4 + dd], 8:16, :] = rest


def scale_kernel(parts, spread, router):
    both = parts[:, :8, :].astype(jnp.float32) + parts[:, 8:16, :].astype(jnp.float32)
    scale = jnp.sum(both, axis=0) / D_MODEL
    for k in range(S // 2):
        low, high = join(parts[PLACE[2 * k], 16:, :], parts[PLACE[2 * k + 1], 16:, :])
        router[:, k * 128 : (k + 1) * 128] = jnp.concatenate([low, high], axis=0)
    for s in range(S):
        spread[s] = scale


def pack_kernel(merged, scales, packed, inverse):
    for j in range(C // 128):
        tiles = regroup([scales[PLACE[4 * j + dd]] for dd in range(4)])
        for g in range(4):
            inverse[g, :, j * 128 : (j + 1) * 128] = 1.0 / tiles[g]

    for j in range(C // 128):
        cols = slice(j * 128, (j + 1) * 128)
        for tp in range(TP):
            halves = []
            for par in range(2):
                te = 2 * tp + par
                factor = inverse[te // 8, te % 8 : te % 8 + 1, cols]
                halves.append((merged[te, :, cols] * factor).astype(jnp.bfloat16))
            turned = jnp.concatenate(halves, axis=0).T
            for dd in range(4):
                rows = slice(tp * W, (tp + 1) * W)
                packed[PLACE[4 * j + dd], rows, :] = turned[dd * W : (dd + 1) * W]


def unpack_kernel(
    arrived, spread, r0, r1, r2, r3, out_gate, out_up, out_router, scale_gate, scale_up, *scratch
):
    joined, scales, out_sems, router_sems, scale_sems = scratch
    me = lax.axis_index("expert")
    routers = (r0, r1, r2, r3)

    def serve(k):
        rows = pl.ds(pl.multiple_of(lax.bitwise_xor(me, k) * E, E), E)
        return pltpu.make_async_copy(routers[k], out_router.at[rows], router_sems.at[k])

    def give(t, p):
        out = (out_gate, out_up)[t]
        return pltpu.make_async_copy(
            joined.at[t, pl.ds(2 * p, 2)], out.at[pl.ds(2 * p, 2)], out_sems.at[t, p]
        )

    def step(p, carry):
        for t in range(2):
            rows = slice((t * PAIRS + p) * W, (t * PAIRS + p + 1) * W)
            for k in range(S // 2):
                cols = slice(k * 128, (k + 1) * 128)
                even, odd = join(arrived[PLACE[2 * k], rows], arrived[PLACE[2 * k + 1], rows])
                joined[t, 2 * p, :, cols] = even
                joined[t, 2 * p + 1, :, cols] = odd
            give(t, p).start()
        return carry

    for p in range(2):
        step(p, 0)
    for k in range(4):
        serve(k).start()
    for g in range(4):
        rows = slice((g % 2) * 8, (g % 2) * 8 + 8)
        scales[g // 2, rows, :] = spread[0, :, g * W : (g + 1) * W]
    scaled = [
        pltpu.make_async_copy(scales.at[t], out, scale_sems.at[t])
        for t, out in enumerate((scale_gate, scale_up))
    ]
    for each in scaled:
        each.start()
    for p in range(2, PAIRS):
        step(p, 0)
    for p in range(PAIRS):
        for t in range(2):
            give(t, p).wait()
    for k in range(4):
        serve(k).wait()
    for each in scaled:
        each.wait()


def whole():
    return pl.BlockSpec(memory_space=pltpu.VMEM)


def remote():
    return pl.BlockSpec(memory_space=pltpu.HBM)


def params(mib):
    return pltpu.CompilerParams(vmem_limit_bytes=mib * MIB)


def exchange(x):
    return lax.all_to_all(
        x, "shard", split_axis=0, concat_axis=0, tiled=True, axis_index_groups=[ORDER]
    )


def serve_step(master_gate, second_gate, master_up, second_up, mix_share, router_weight, router_gain):
    merged, sums = pl.pallas_call(
        merge_kernel,
        in_specs=[remote()] * 7,
        out_specs=[whole(), whole()],
        out_shape=[
            pltpu.VMEM((2 * E, R, C), jnp.float32),
            pltpu.VMEM((S, 24, 128), jnp.bfloat16),
        ],
        scratch_shapes=[
            pltpu.VMEM((4, E, R, C), jnp.float32),
            pltpu.VMEM((4, 8, C), jnp.float32),
            pltpu.SMEM((E,), jnp.float32),
            pltpu.VMEM((E, R), jnp.float32),
            pltpu.VMEM((1, R), jnp.float32),
            pltpu.SemaphoreType.DMA((4, PAIRS)),
            pltpu.SemaphoreType.DMA((3,)),
        ],
        compiler_params=params(20),
        name="merge",
    )(
        *(
            pltpu.with_memory_space_constraint(x, pltpu.HBM)
            for x in (mix_share, master_gate, second_gate, master_up, second_up)
        ),
        pltpu.with_memory_space_constraint(router_weight.T, pltpu.HBM),
        pltpu.with_memory_space_constraint(router_gain[None, :], pltpu.HBM),
    )

    parts = exchange(sums)

    spread, router = pl.pallas_call(
        scale_kernel,
        in_specs=[whole()],
        out_specs=[whole()] * 2,
        out_shape=[
            pltpu.VMEM((S, 8, 128), jnp.float32),
            pltpu.VMEM((E, S * R), jnp.bfloat16),
        ],
        compiler_params=params(4),
        name="scale",
    )(parts)
    hops = [
        lax.ppermute(router, "expert", [(z, z ^ k) for z in range(4)])
        for k in range(1, 4)
    ]
    scales = exchange(spread)

    packed = pl.pallas_call(
        pack_kernel,
        in_specs=[whole()] * 2,
        out_specs=whole(),
        out_shape=pltpu.VMEM((S, TP * W, 128), jnp.bfloat16),
        scratch_shapes=[pltpu.VMEM((4, 8, C), jnp.float32)],
        compiler_params=params(4),
        name="pack",
    )(merged, scales)
    arrived = pltpu.with_memory_space_constraint(exchange(packed), pltpu.VMEM)

    final_gate, final_up, serve_router, scale_gate, scale_up = pl.pallas_call(
        unpack_kernel,
        in_specs=[whole()] * 6,
        out_specs=[remote()] * 5,
        out_shape=[jax.ShapeDtypeStruct((E, W, S * R), jnp.bfloat16)] * 2
        + [jax.ShapeDtypeStruct((4 * E, S * R), jnp.bfloat16)]
        + [jax.ShapeDtypeStruct((E, W), jnp.float32)] * 2,
        scratch_shapes=[
            pltpu.VMEM((2, E, W, S * R), jnp.bfloat16),
            pltpu.VMEM((2, E, W), jnp.float32),
            pltpu.SemaphoreType.DMA((2, PAIRS)),
            pltpu.SemaphoreType.DMA((4,)),
            pltpu.SemaphoreType.DMA((2,)),
        ],
        compiler_params=params(10),
        name="unpack",
    )(arrived, spread, router, *hops)
    return (
        final_gate.transpose(0, 2, 1),
        final_up.transpose(0, 2, 1),
        scale_gate,
        scale_up,
        serve_router.T,
    )


def solution(mesh):
    in_specs = (
        P("expert", "shard", None),
        P("expert", "shard", None),
        P("expert", "shard", None),
        P("expert", "shard", None),
        P("expert"),
        P("shard", "expert"),
        P("shard"),
    )
    out_specs = (
        P("expert", None, "shard"),
        P("expert", None, "shard"),
        P("expert", "shard"),
        P("expert", "shard"),
        P(),
    )
    return jax.shard_map(serve_step, mesh=mesh, in_specs=in_specs, out_specs=out_specs, check_vma=False)
```
